8 devices in a mesh: dp: 1 (over z), tp: 8 (over x, y, core).
Axes of the slice: x: 2, y: 2, z: 1, core: 2. Of those that a mesh axis runs over, the one named last changes fastest.
Arguments:
- x: bfloat16 [3072, 3072], P(('dp', 'tp'))
- gain: bfloat16 [3072], replicated
- wq: bfloat16 [3072, 4096], P(None, 'tp')
- wk: bfloat16 [3072, 4096], P(None, 'tp')
- wv: bfloat16 [3072, 4096], P(None, 'tp')
- wo: bfloat16 [4096, 3072], P('tp')
Outputs:
- output: bfloat16 [3072, 3072], P(('dp', 'tp'))
All inputs are finite; a program needn't handle non-finite values.
Results may differ from the reference program's by a relative error of at most 0.012.
Values are sent between devices in bfloat16 or wider.
A program may use at most 2 GiB of HBM per device.

```python
import jax
import jax.numpy as jnp
from jax import lax

ROWS = 3072
D = 3072
HEADS = 16
KV_HEADS = 16
HEAD = 256
THETA = 10000


def setup_inputs(seed: int = 0, part: int = 0) -> dict:
    kx, kn, kq, kk, kv, ko = jax.random.split(jax.random.key(seed), 6)

    def weights(key, rows, columns):
        return jax.random.normal(key, (rows, columns), jnp.float32) * rows**-0.5

    drawn = {
        "x": jax.random.normal(jax.random.fold_in(kx, part), (ROWS, D), jnp.float32),
        "gain": 1 + 0.1 * jax.random.normal(kn, (D,), jnp.float32),
        "wq": 2 * weights(kq, D, HEADS * HEAD),
        "wk": 2 * weights(kk, D, KV_HEADS * HEAD),
        "wv": 4 * weights(kv, D, KV_HEADS * HEAD),
        "wo": weights(ko, HEADS * HEAD, D),
    }
    return {k: v.astype(jnp.bfloat16) for k, v in drawn.items()}


def normed(x, gain):
    wide = x.astype(jnp.float32)
    scale = lax.rsqrt(jnp.mean(wide * wide, -1, keepdims=True) + 1e-6)
    return (wide * scale * gain.astype(jnp.float32)).astype(jnp.bfloat16)


def turned(t, place, theta):
    half = t.shape[-1] // 2
    angle = place.astype(jnp.float32)[:, None] * theta ** (-jnp.arange(half, dtype=jnp.float32) / half)
    cos, sin = jnp.cos(angle)[:, None], jnp.sin(angle)[:, None]
    a, b = t[..., :half].astype(jnp.float32), t[..., half:].astype(jnp.float32)
    return jnp.concatenate([a * cos - b * sin, b * cos + a * sin], -1).astype(jnp.bfloat16)


def matmul(a, w):
    return jnp.dot(a, w, preferred_element_type=jnp.float32).astype(jnp.bfloat16)


def einsum(form, a, b):
    return jnp.einsum(form, a.astype(jnp.float32), b.astype(jnp.float32))


def attention(q, k, v):
    scores = einsum("tgsd,ugd->gstu", q, k) * q.shape[-1] ** -0.5
    token = jnp.arange(q.shape[0])
    scores = jnp.where(token[:, None] >= token, scores, -jnp.inf)
    weights = jax.nn.softmax(scores, -1).astype(jnp.bfloat16)
    return einsum("gstu,ugd->tgsd", weights, v).astype(jnp.bfloat16)


def reference(x, gain, wq, wk, wv, wo):
    a, place = normed(x, gain), jnp.arange(ROWS)
    q = turned(matmul(a, wq).reshape(ROWS, HEADS, HEAD), place, THETA).reshape(ROWS, KV_HEADS, -1, HEAD)
    k = turned(matmul(a, wk).reshape(ROWS, KV_HEADS, HEAD), place, THETA)
    v = matmul(a, wv).reshape(ROWS, KV_HEADS, HEAD)
    seen = attention(q, k, v).reshape(ROWS, HEADS * HEAD)
    return (x.astype(jnp.float32) + jnp.dot(seen, wo, preferred_element_type=jnp.float32)).astype(jnp.bfloat16)
```

```python
import functools

import jax
import jax.numpy as jnp
from jax import lax
from jax.experimental import pallas as pl
from jax.experimental.pallas import tpu as pltpu
from jax.sharding import PartitionSpec as P

HEAD = 256
THETA = 10000
LOG2E = 1.4426950408889634
NEG = -1e30
EPS = 1e-6
CH = 128
NCH = 3
ROWS = CH * NCH
D = 3072
HALF = D // 2
TILE = 512
HT = HALF // TILE
SEQ = 8 * ROWS
CHIP = 2 * ROWS
STRIP = 256
NS = CHIP // STRIP
SUMS = 16
WIDTH = 2 * HEAD
SCALE = HEAD**-0.5
E2 = SCALE * LOG2E

f32, bf16 = jnp.float32, jnp.bfloat16


def dot(a, b, ca=1, cb=0):
    return lax.dot_general(a, b, (((ca,), (cb,)), ((), ())), preferred_element_type=f32)


def kernel(x_ref, gain_ref, wq_ref, wk_ref, wv_ref, wo_ref, near_ref, far_ref, o_ref,
           xr, xg, w, wo, q, k, vt, pb, rd, rx, ry, top_s, mix_s,
           load, own_s, arr, fwd_s, arr2, wo_s, ex_s, rs_s, rs_r, out_s):
    me = lax.axis_index("tp")
    chip = me // 2
    core = me - 2 * chip
    chip_x = lax.rem(chip + 2, 4)
    chip_y = chip + 1 - 2 * lax.rem(chip, 2)
    chip_d = 3 - chip
    other, dev_x, dev_y = 2 * chip + 1 - core, 2 * chip_x + core, 2 * chip_y + core

    def remote(src, dst, s, r, to):
        return pltpu.make_async_remote_copy(src_ref=src, dst_ref=dst, send_sem=s, recv_sem=r, device_id={"tp": to},
                                            device_id_type=pl.DeviceIdType.MESH)

    lx = pltpu.make_async_copy(x_ref, xr, load.at[0])
    lx.start()
    lws = [pltpu.make_async_copy(r, w.at[i], load.at[1 + i]) for i, r in enumerate((wq_ref, wk_ref, wv_ref))]
    for c in lws:
        c.start()
    lwo = pltpu.make_async_copy(wo_ref, wo.at[0:WIDTH], load.at[4])
    lwo.start()

    barrier = pltpu.get_barrier_semaphore()
    for to in (other, dev_x, dev_y):
        pl.semaphore_signal(barrier, inc=1, device_id={"tp": to}, device_id_type=pl.DeviceIdType.MESH)
    lx.wait()

    def piece(p):
        return pl.ds(pl.multiple_of(p * CH, CH), CH)

    def nbr(j, i):
        return 2 * NCH + 4 * j + i

    def diag(j, i):
        return 6 * NCH + 2 * j + i

    def own_other(j):
        return remote(xg.at[piece(j)], xg.at[piece(NCH + j)], own_s.at[0, j], arr.at[0, j], other)

    def own_x(j):
        return remote(xg.at[piece(j)], xg.at[piece(nbr(j, 0))], own_s.at[1, j], arr.at[1, j], dev_x)

    def own_y(j):
        return remote(xg.at[piece(j)], xg.at[piece(nbr(j, 2))], own_s.at[2, j], arr.at[2, j], dev_y)

    def x_other(j):
        return remote(xg.at[piece(nbr(j, 0))], xg.at[piece(nbr(j, 1))], fwd_s.at[0, j], arr2.at[0, j], other)

    def y_other(j):
        return remote(xg.at[piece(nbr(j, 2))], xg.at[piece(nbr(j, 3))], fwd_s.at[1, j], arr2.at[1, j], other)

    def x_on(j):
        return remote(xg.at[piece(nbr(j, 0)), 0:HALF], xg.at[piece(diag(j, 0)), 0:HALF], fwd_s.at[2, j], arr2.at[2, j], dev_y)

    def y_on(j):
        return remote(xg.at[piece(nbr(j, 2)), HALF:D], xg.at[piece(diag(j, 0)), HALF:D], fwd_s.at[3, j], arr2.at[3, j], dev_x)

    def d_other(j):
        return remote(xg.at[piece(diag(j, 0))], xg.at[piece(diag(j, 1))], fwd_s.at[4, j], arr2.at[4, j], other)

    gain = gain_ref[...].astype(f32)
    SUB = 32

    def norm(i, _):
        rows = pl.ds(pl.multiple_of(i * SUB, SUB), SUB)
        wide = xr[rows, :].astype(f32)
        scale = lax.rsqrt(jnp.mean(wide * wide, -1, keepdims=True) + EPS)
        xg[rows, :] = (wide * scale * gain).astype(bf16)

    per = CH // SUB
    lax.fori_loop(0, per, norm, None)
    pl.semaphore_wait(barrier, 3)
    for j in range(NCH):
        own_x(j).start()
        own_y(j).start()
        own_other(j).start()
        if j + 1 < NCH:
            lax.fori_loop((j + 1) * per, (j + 2) * per, norm, None)
    wo_copy = remote(wo_ref, wo.at[WIDTH : 2 * WIDTH], wo_s.at[0], wo_s.at[1], other)
    wo_copy.start()
    for h in range(2):
        vt[h, HEAD : HEAD + SUMS, :] = jnp.ones((SUMS, SEQ), bf16)
    for c in lws:
        c.wait()

    def chunk_of(p):
        mine, theirs = 2 * chip + core, 2 * chip + 1 - core
        n = jnp.maximum(p - 2 * NCH, 0)
        nj, ni = n // 4, lax.rem(n, 4)
        nd = 2 * jnp.where(ni < 2, chip_x, chip_y) + jnp.where(lax.rem(ni, 2) == 0, core, 1 - core)
        m = jnp.maximum(p - 6 * NCH, 0)
        mj, mi = m // 2, lax.rem(m, 2)
        md = 2 * chip_d + jnp.where(mi == 0, core, 1 - core)
        at = jnp.where(p < NCH, mine * NCH + p, theirs * NCH + p - NCH)
        at = jnp.where(p >= 2 * NCH, nd * NCH + nj, at)
        return jnp.where(p >= 6 * NCH, md * NCH + mj, at)

    def project(b, _):
        @pl.when(b == 1)
        def _():
            own_other(0).wait_recv()

        @pl.when(b == 2)
        def _():
            own_other(1).wait_recv()
            own_other(2).wait_recv()

        for j in range(NCH):

            @pl.when(b == NCH + 2 * j)
            def _():
                own_x(j).wait_recv()
                x_other(j).start()
                x_on(j).start()
                own_y(j).wait_recv()
                y_other(j).start()
                y_on(j).start()
                x_other(j).wait_recv()

            @pl.when(b == NCH + 2 * j + 1)
            def _():
                y_other(j).wait_recv()

            @pl.when(b == 3 * NCH + j)
            def _():
                x_on(j).wait_recv()
                y_on(j).wait_recv()
                d_other(j).start()
                d_other(j).wait_recv()

        rows = xg[pl.ds(pl.multiple_of(b * 2 * CH, 2 * CH), 2 * CH), :]
        places, trig = [], []
        for i in range(2):
            at = chunk_of(2 * b + i)
            places.append(pl.ds(pl.multiple_of(at * CH, CH), CH))
            cf, sf = far_ref[0, pl.ds(at, 1), :], far_ref[1, pl.ds(at, 1), :]
            cn, sn = near_ref[0], near_ref[1]
            trig.append((cf * cn - sf * sn, sf * cn + cf * sn))
        for n, to in ((0, q), (1, k)):
            for h in range(2):
                t = dot(rows, w[n, :, h * HEAD : (h + 1) * HEAD]).astype(bf16).astype(f32)
                for i in range(2):
                    a, b_ = t[i * CH : (i + 1) * CH, : HEAD // 2], t[i * CH : (i + 1) * CH, HEAD // 2 :]
                    cos, sin = trig[i]
                    to[h, places[i], :] = jnp.concatenate([a * cos - b_ * sin, b_ * cos + a * sin], -1).astype(bf16)
        for h in range(2):
            t = dot(rows, w[2, :, h * HEAD : (h + 1) * HEAD]).astype(bf16)
            for i in range(2):
                vt[h, 0:HEAD, places[i]] = t[i * CH : (i + 1) * CH].T

    lax.fori_loop(0, 4 * NCH, project, None)

    for j in range(NCH):
        for c in (own_other, own_x, own_y, x_other, y_other, x_on, y_on, d_other):
            c(j).wait_send()
    lwo.wait()
    wo_copy.wait()

    def results(i, of):
        return pl.ds(pl.multiple_of(i * CHIP + of * ROWS, ROWS), ROWS)

    pieces = [(h, s) for h in range(2) for s in range(NS)]

    def attention(i, to):
        q0 = pl.multiple_of(to * CHIP, CHIP)
        for n in range(2 * NS):
            top_s[n : n + 1, :] = jnp.full((1, STRIP), NEG, f32)
        mix_s[...] = jnp.zeros(mix_s.shape, f32)

        def block(k0, masked):
            scores = []
            for h, s in pieces:
                keys = (s + 1) * STRIP if masked else CHIP
                qs = q[h, pl.ds(q0 + s * STRIP, STRIP), :]
                scores.append(dot(k[h, pl.ds(k0, keys), :], qs, 1, 1))
            weights, keeps = [], []
            for n, ((h, s), sc) in enumerate(zip(pieces, scores)):
                if masked:
                    ok = (lax.broadcasted_iota(jnp.int32, sc.shape, 0) - s * STRIP) <= lax.broadcasted_iota(jnp.int32, sc.shape, 1)
                    sc = jnp.where(ok, sc, 2 * NEG)
                old = top_s[n : n + 1, :]
                top = jnp.maximum(old, sc.max(axis=0, keepdims=True))
                top_s[n : n + 1, :] = top
                weights.append(jnp.exp2((sc - top) * E2).astype(bf16))
                keeps.append(jnp.exp2((old - top) * E2))
            for n, (h, s) in enumerate(pieces):
                keys = (s + 1) * STRIP if masked else CHIP
                mix_s[n] = mix_s[n] * keeps[n] + dot(vt[h, :, pl.ds(k0, keys)], weights[n])

        lax.fori_loop(0, to, lambda j, _: block(pl.multiple_of(j * CHIP, CHIP), False), None)
        block(q0, True)
        for n, (h, s) in enumerate(pieces):
            out = mix_s[n, 0:HEAD, :] * (1 / mix_s[n, HEAD : HEAD + 1, :])
            w[0, pl.ds(pl.multiple_of(i * CHIP + s * STRIP, STRIP), STRIP), h * HEAD : (h + 1) * HEAD] = out.T.astype(bf16)

    def exchange(i):
        return remote(w.at[0, results(i, 1 - core), :], pb.at[i], ex_s.at[0, i], ex_s.at[1, i], other)

    def term(i, t):
        mine = w[0, results(i, core), :]
        cols = pl.ds(pl.multiple_of(t * TILE, TILE), TILE)
        return dot(jnp.concatenate([mine, pb[i]], axis=1), wo[:, cols])

    def cols(t):
        return pl.ds(pl.multiple_of(t * TILE, TILE), TILE)

    SX, SY, SD = (slice(n * ROWS, (n + 1) * ROWS) for n in range(3))

    def send_x(t):
        return remote(xg.at[SX, cols(t)], rx.at[:, cols(t)], rs_s.at[0, t], rs_r.at[0, t], dev_x)

    def send_y(t):
        return remote(xg.at[SY, cols(t)], ry.at[:, cols(t)], rs_s.at[1, t], rs_r.at[1, t], dev_y)

    def send_d(t):
        return remote(xg.at[SD, cols(t)], rd.at[:, cols(t)], rs_s.at[2, t], rs_r.at[2, t], dev_x)

    def send_e(t):
        return remote(xg.at[SD, cols(t)], rd.at[:, cols(t)], rs_s.at[2, t], rs_r.at[2, t], dev_y)

    def item(i, _):
        to = jnp.where(i == 0, chip_x, jnp.where(i == 1, chip_y, jnp.where(i == 2, chip_d, chip)))
        attention(i, to)
        ex = exchange(i)
        ex.start()
        ex.wait_recv()

        def direct(t, _):
            tx, ty = t, HT + t

            @pl.when(i == 0)
            def _():
                xg[SX, cols(tx)] = term(0, tx).astype(bf16)
                send_x(tx).start()

            @pl.when(i == 1)
            def _():
                xg[SY, cols(ty)] = term(1, ty).astype(bf16)
                send_y(ty).start()

            @pl.when(i == 2)
            def _():
                xg[SD, cols(tx)] = term(2, tx).astype(bf16)
                send_d(tx).start()
                xg[SD, cols(ty)] = term(2, ty).astype(bf16)
                send_e(ty).start()

        lax.fori_loop(0, jnp.where(i == 3, 0, HT), direct, None)

    lax.fori_loop(0, 4, item, None)

    def combine(t, _):
        tx, ty = HT + t, t
        send_e(tx).wait_recv()
        xg[SX, cols(tx)] = (term(0, tx) + rd[:, cols(tx)].astype(f32)).astype(bf16)
        send_x(tx).start()
        send_d(ty).wait_recv()
        xg[SY, cols(ty)] = (term(1, ty) + rd[:, cols(ty)].astype(f32)).astype(bf16)
        send_y(ty).start()

    lax.fori_loop(0, HT, combine, None)

    def finish(n, _):
        t = n // 2 + HT * lax.rem(n, 2)
        send_x(t).wait_recv()
        send_y(t).wait_recv()
        total = term(3, t) + rx[:, cols(t)].astype(f32) + ry[:, cols(t)].astype(f32)
        xr[:, cols(t)] = (xr[:, cols(t)].astype(f32) + total).astype(bf16)
        pltpu.make_async_copy(xr.at[:, cols(t)], o_ref.at[:, cols(t)], out_s.at[t]).start()

    lax.fori_loop(0, 2 * HT, finish, None)
    for t in range(2 * HT):
        send_x(t).wait_send()
        send_y(t).wait_send()
        (send_d if t < HT else send_e)(t).wait_send()
        pltpu.make_async_copy(xr.at[:, cols(t)], o_ref.at[:, cols(t)], out_s.at[t]).wait()
    for i in range(4):
        exchange(i).wait_send()


def solution(mesh):
    def step(x, gain, wq, wk, wv, wo):
        rate = THETA ** (-jnp.arange(HEAD // 2, dtype=f32) / (HEAD // 2))
        near = jnp.arange(CH, dtype=f32)[:, None] * rate
        far = (jnp.arange(SEQ // CH, dtype=f32) * CH)[:, None] * rate
        vmem, hbm = pl.BlockSpec(memory_space=pltpu.VMEM), pl.BlockSpec(memory_space=pl.ANY)
        dma, V = pltpu.SemaphoreType.DMA, pltpu.VMEM
        return pl.pallas_call(
            kernel,
            out_shape=jax.ShapeDtypeStruct((ROWS, D), bf16),
            in_specs=[hbm, vmem, hbm, hbm, hbm, hbm, vmem, vmem],
            out_specs=hbm,
            scratch_shapes=[
                V((ROWS, D), bf16),
                V((SEQ, D), bf16),
                V((3, D, WIDTH), bf16),
                V((2 * WIDTH, D), bf16),
                V((2, SEQ, HEAD), bf16),
                V((2, SEQ, HEAD), bf16),
                V((2, HEAD + SUMS, SEQ), bf16),
                V((4, ROWS, WIDTH), bf16),
                V((ROWS, D), bf16),
                V((ROWS, D), bf16),
                V((ROWS, D), bf16),
                V((8, STRIP), f32),
                V((2 * NS, HEAD + SUMS, STRIP), f32),
                dma((5,)), dma((3, NCH)), dma((3, NCH)), dma((5, NCH)), dma((5, NCH)), dma((2,)), dma((2, 4)),
                dma((3, 2 * HT)), dma((3, 2 * HT)), dma((2 * HT,)),
            ],
            compiler_params=pltpu.CompilerParams(collective_id=0, has_side_effects=True, vmem_limit_bytes=67043328),
        )(x, gain[None], wq, wk, wv, wo, jnp.stack([jnp.cos(near), jnp.sin(near)]), jnp.stack([jnp.cos(far), jnp.sin(far)]))

    tokens, columns = P(("dp", "tp"), None), P(None, "tp")
    return jax.shard_map(
        step,
        mesh=mesh,
        in_specs=(tokens, P(None), columns, columns, columns, P("tp", None)),
        out_specs=tokens,
        check_vma=False,
    )
```

```python
import functools

import jax
import jax.numpy as jnp
import numpy as np
from jax import lax
from jax.experimental import pallas as pl
from jax.experimental.pallas import tpu as pltpu
from jax.sharding import PartitionSpec as P

HEAD = 256
THETA = 10000
LOG2E = 1.4426950408889634
NEG = -1e30
EPS = 1e-6
CH = 128
NCH = 3
ROWS = CH * NCH
D = 3072
HALF = D // 2
TILE = 512
HT = HALF // TILE
SEQ = 8 * ROWS
CHIP = 2 * ROWS
STRIP = 256
NS = CHIP // STRIP
SUMS = 16
WIDTH = 2 * HEAD
SCALE = HEAD**-0.5
E2 = SCALE * LOG2E

f32, bf16 = jnp.float32, jnp.bfloat16


def dot(a, b, ca=1, cb=0):
    return lax.dot_general(a, b, (((ca,), (cb,)), ((), ())), preferred_element_type=f32)


def kernel(x_ref, gain_ref, wq_ref, wk_ref, wv_ref, wo_ref, near_ref, far_ref, o_ref,
           xr, xg, w, wo, q, k, vt, pb, rd, rx, ry, top_s, mix_s, gain_v, near_v, far_v,
           load, own_s, arr, fwd_s, arr2, wo_s, ex_s, rs_s, rs_r, out_s):
    me = lax.axis_index("tp")
    chip = me // 2
    core = me - 2 * chip
    chip_x = lax.rem(chip + 2, 4)
    chip_y = chip + 1 - 2 * lax.rem(chip, 2)
    chip_d = 3 - chip
    other, dev_x, dev_y = 2 * chip + 1 - core, 2 * chip_x + core, 2 * chip_y + core

    def remote(src, dst, s, r, to):
        return pltpu.make_async_remote_copy(src_ref=src, dst_ref=dst, send_sem=s, recv_sem=r, device_id={"tp": to},
                                            device_id_type=pl.DeviceIdType.MESH)

    lgain = pltpu.make_async_copy(gain_ref, gain_v, load.at[5])
    lgain.start()
    lxs = [pltpu.make_async_copy(x_ref.at[j * CH : (j + 1) * CH], xr.at[j * CH : (j + 1) * CH], load.at[8 + j]) for j in range(NCH)]
    for c in lxs:
        c.start()
    lnear, lfar = pltpu.make_async_copy(near_ref, near_v, load.at[6]), pltpu.make_async_copy(far_ref, far_v, load.at[7])
    lnear.start()
    lfar.start()
    lws = [pltpu.make_async_copy(r, w.at[i], load.at[1 + i]) for i, r in enumerate((wq_ref, wk_ref, wv_ref))]
    for c in lws:
        c.start()
    lwo = pltpu.make_async_copy(wo_ref, wo.at[0:WIDTH], load.at[4])
    lwo.start()

    barrier = pltpu.get_barrier_semaphore()
    for to in (other, dev_x, dev_y):
        pl.semaphore_signal(barrier, inc=1, device_id={"tp": to}, device_id_type=pl.DeviceIdType.MESH)
    lgain.wait()
    lxs[0].wait()

    def piece(p):
        return pl.ds(pl.multiple_of(p * CH, CH), CH)

    def nbr(j, i):
        return 2 * NCH + 4 * j + i

    def diag(j, i):
        return 6 * NCH + 2 * j + i

    def own_other(j):
        return remote(xg.at[piece(j)], xg.at[piece(NCH + j)], own_s.at[0, j], arr.at[0, j], other)

    def own_x(j):
        return remote(xg.at[piece(j)], xg.at[piece(nbr(j, 0))], own_s.at[1, j], arr.at[1, j], dev_x)

    def own_y(j):
        return remote(xg.at[piece(j)], xg.at[piece(nbr(j, 2))], own_s.at[2, j], arr.at[2, j], dev_y)

    def x_other(j):
        return remote(xg.at[piece(nbr(j, 0))], xg.at[piece(nbr(j, 1))], fwd_s.at[0, j], arr2.at[0, j], other)

    def y_other(j):
        return remote(xg.at[piece(nbr(j, 2))], xg.at[piece(nbr(j, 3))], fwd_s.at[1, j], arr2.at[1, j], other)

    def x_on(j):
        return remote(xg.at[piece(nbr(j, 0)), 0:HALF], xg.at[piece(diag(j, 0)), 0:HALF], fwd_s.at[2, j], arr2.at[2, j], dev_y)

    def y_on(j):
        return remote(xg.at[piece(nbr(j, 2)), HALF:D], xg.at[piece(diag(j, 0)), HALF:D], fwd_s.at[3, j], arr2.at[3, j], dev_x)

    def d_other(j):
        return remote(xg.at[piece(diag(j, 0))], xg.at[piece(diag(j, 1))], fwd_s.at[4, j], arr2.at[4, j], other)

    gain = gain_v[...].reshape(1, D).astype(f32)
    SUB = 32

    def norm(i, _):
        rows = pl.ds(pl.multiple_of(i * SUB, SUB), SUB)
        wide = xr[rows, :].astype(f32)
        scale = lax.rsqrt(jnp.mean(wide * wide, -1, keepdims=True) + EPS)
        xg[rows, :] = (wide * scale * gain).astype(bf16)

    per = CH // SUB
    lax.fori_loop(0, per, norm, None)
    pl.semaphore_wait(barrier, 3)
    for j in range(NCH):
        own_x(j).start()
        own_y(j).start()
        own_other(j).start()
        if j + 1 < NCH:
            lxs[j + 1].wait()
            lax.fori_loop((j + 1) * per, (j + 2) * per, norm, None)
    wo_copy = remote(wo_ref, wo.at[WIDTH : 2 * WIDTH], wo_s.at[0], wo_s.at[1], other)
    wo_copy.start()
    for h in range(2):
        vt[h, HEAD : HEAD + SUMS, :] = jnp.ones((SUMS, SEQ), bf16)
    for c in (*lws, lnear, lfar):
        c.wait()

    def chunk_of(p):
        mine, theirs = 2 * chip + core, 2 * chip + 1 - core
        n = jnp.maximum(p - 2 * NCH, 0)
        nj, ni = n // 4, lax.rem(n, 4)
        nd = 2 * jnp.where(ni < 2, chip_x, chip_y) + jnp.where(lax.rem(ni, 2) == 0, core, 1 - core)
        m = jnp.maximum(p - 6 * NCH, 0)
        mj, mi = m // 2, lax.rem(m, 2)
        md = 2 * chip_d + jnp.where(mi == 0, core, 1 - core)
        at = jnp.where(p < NCH, mine * NCH + p, theirs * NCH + p - NCH)
        at = jnp.where(p >= 2 * NCH, nd * NCH + nj, at)
        return jnp.where(p >= 6 * NCH, md * NCH + mj, at)

    def project(b):
        @pl.when(b == 1)
        def _():
            own_other(0).wait_recv()

        @pl.when(b == 2)
        def _():
            own_other(1).wait_recv()
            own_other(2).wait_recv()

        for j in range(NCH):

            @pl.when(b == NCH + 2 * j)
            def _():
                own_x(j).wait_recv()
                x_other(j).start()
                x_on(j).start()
                own_y(j).wait_recv()
                y_other(j).start()
                y_on(j).start()
                x_other(j).wait_recv()

            @pl.when(b == NCH + 2 * j + 1)
            def _():
                y_other(j).wait_recv()

            @pl.when(b == 3 * NCH + j)
            def _():
                x_on(j).wait_recv()
                y_on(j).wait_recv()
                d_other(j).start()
                d_other(j).wait_recv()

        rows = xg[pl.ds(pl.multiple_of(b * 2 * CH, 2 * CH), 2 * CH), :]
        places, trig = [], []
        for i in range(2):
            at = chunk_of(2 * b + i)
            places.append(pl.ds(pl.multiple_of(at * CH, CH), CH))
            cf, sf = far_v[0, pl.ds(at, 1), :], far_v[1, pl.ds(at, 1), :]
            cn, sn = near_v[0], near_v[1]
            trig.append((cf * cn - sf * sn, sf * cn + cf * sn))
        for n, to in ((0, q), (1, k)):
            for h in range(2):
                t = dot(rows, w[n, :, h * HEAD : (h + 1) * HEAD]).astype(bf16).astype(f32)
                for i in range(2):
                    a, b_ = t[i * CH : (i + 1) * CH, : HEAD // 2], t[i * CH : (i + 1) * CH, HEAD // 2 :]
                    cos, sin = trig[i]
                    to[h, places[i], :] = jnp.concatenate([a * cos - b_ * sin, b_ * cos + a * sin], -1).astype(bf16)
        for h in range(2):
            t = dot(rows, w[2, :, h * HEAD : (h + 1) * HEAD]).astype(bf16)
            for i in range(2):
                vt[h, 0:HEAD, places[i]] = t[i * CH : (i + 1) * CH].T

    def place(i):
        return pl.ds(pl.multiple_of(i * WIDTH, WIDTH), WIDTH)

    def results(of):
        return pl.ds(pl.multiple_of(of * ROWS, ROWS), ROWS)

    pieces = [(h, s) for h in range(2) for s in range(NS)]

    def attention(i, to):
        q0 = pl.multiple_of(to * CHIP, CHIP)
        for n in range(2 * NS):
            top_s[n : n + 1, :] = jnp.full((1, STRIP), NEG, f32)
        mix_s[...] = jnp.zeros(mix_s.shape, f32)

        def block(k0, masked):
            scores = []
            for h, s in pieces:
                keys = (s + 1) * STRIP if masked else CHIP
                qs = q[h, pl.ds(q0 + s * STRIP, STRIP), :]
                scores.append(dot(k[h, pl.ds(k0, keys), :], qs, 1, 1))
            weights, keeps = [], []
            for n, ((h, s), sc) in enumerate(zip(pieces, scores)):
                if masked:
                    ok = (lax.broadcasted_iota(jnp.int32, sc.shape, 0) - s * STRIP) <= lax.broadcasted_iota(jnp.int32, sc.shape, 1)
                    sc = jnp.where(ok, sc, 2 * NEG)
                old = top_s[n : n + 1, :]
                top = jnp.maximum(old, sc.max(axis=0, keepdims=True))
                top_s[n : n + 1, :] = top
                weights.append(jnp.exp2((sc - top) * E2).astype(bf16))
                keeps.append(jnp.exp2((old - top) * E2))
            for n, (h, s) in enumerate(pieces):
                keys = (s + 1) * STRIP if masked else CHIP
                mix_s[n] = mix_s[n] * keeps[n] + dot(vt[h, :, pl.ds(k0, keys)], weights[n])

        lax.fori_loop(0, to, lambda j, _: block(pl.multiple_of(j * CHIP, CHIP), False), None)
        block(q0, True)
        for n, (h, s) in enumerate(pieces):
            out = mix_s[n, 0:HEAD, :] * (1 / mix_s[n, HEAD : HEAD + 1, :])
            xg[s * STRIP : (s + 1) * STRIP, pl.ds(pl.multiple_of(i * WIDTH + h * HEAD, HEAD), HEAD)] = out.T.astype(bf16)

    def exchange(i):
        return remote(xg.at[results(1 - core), place(i)], pb.at[i], ex_s.at[0, i], ex_s.at[1, i], other)

    def term(i, t):
        mine = xg[results(core), place(i)]
        cols = pl.ds(pl.multiple_of(t * TILE, TILE), TILE)
        return dot(jnp.concatenate([mine, pb[i]], axis=1), wo[:, cols])

    def cols(t):
        return pl.ds(pl.multiple_of(t * TILE, TILE), TILE)

    SX, SY, SD = (slice(n * ROWS, (n + 1) * ROWS) for n in range(2, 5))

    def send_x(t):
        return remote(xg.at[SX, cols(t)], rx.at[:, cols(t)], rs_s.at[0, t], rs_r.at[0, t], dev_x)

    def send_y(t):
        return remote(xg.at[SY, cols(t)], ry.at[:, cols(t)], rs_s.at[1, t], rs_r.at[1, t], dev_y)

    def send_d(t):
        return remote(xg.at[SD, cols(t)], rd.at[:, cols(t)], rs_s.at[2, t], rs_r.at[2, t], dev_x)

    def send_e(t):
        return remote(xg.at[SD, cols(t)], rd.at[:, cols(t)], rs_s.at[2, t], rs_r.at[2, t], dev_y)

    def item(n):
        to = jnp.where(n == 3, chip, n + jnp.where(n >= chip, 1, 0))
        i = jnp.where(to == chip_x, 0, jnp.where(to == chip_y, 1, jnp.where(to == chip_d, 2, 3)))
        attention(i, to)
        ex = exchange(i)
        ex.start()

        @pl.when(n == 0)
        def _():
            for j in range(2):
                for c in (x_other, y_other, x_on, y_on):
                    c(j).wait_send()

        ex.wait_recv()

        def direct(t, _):
            tx, ty = t, HT + t

            @pl.when(i == 0)
            def _():
                xg[SX, cols(tx)] = term(0, tx).astype(bf16)
                send_x(tx).start()

            @pl.when(i == 1)
            def _():
                xg[SY, cols(ty)] = term(1, ty).astype(bf16)
                send_y(ty).start()

            @pl.when(i == 2)
            def _():
                xg[SD, cols(tx)] = term(2, tx).astype(bf16)
                send_d(tx).start()
                xg[SD, cols(ty)] = term(2, ty).astype(bf16)
                send_e(ty).start()

        lax.fori_loop(0, jnp.where(i == 3, 0, HT), direct, None)

    early = jnp.where(chip == 0, 2, jnp.where(chip == 3, 0, 1))
    first = 3 * NCH

    def step(n, _):
        @pl.when(n == first)
        def _():
            lwo.wait()
            wo_copy.wait()
            for j in range(NCH):
                for c in (own_other, own_x, own_y):
                    c(j).wait_send()

        is_item = ((n >= first) & (n < first + early)) | (n >= 4 * NCH + early)

        @pl.when(jnp.logical_not(is_item))
        def _():
            project(jnp.where(n < first, n, n - early))

        @pl.when(n == 4 * NCH + early)
        def _():
            for c in (x_other, y_other, x_on, y_on):
                c(NCH - 1).wait_send()
            for j in range(NCH):
                d_other(j).wait_send()

        @pl.when(is_item)
        def _():
            item(n - jnp.where(n < first + early, first, 4 * NCH))

    lax.fori_loop(0, 4 * NCH + 4, step, None)

    def combine(t, _):
        tx, ty = HT + t, t
        send_e(tx).wait_recv()
        xg[SX, cols(tx)] = (term(0, tx) + rd[:, cols(tx)].astype(f32)).astype(bf16)
        send_x(tx).start()
        send_d(ty).wait_recv()
        xg[SY, cols(ty)] = (term(1, ty) + rd[:, cols(ty)].astype(f32)).astype(bf16)
        send_y(ty).start()

    lax.fori_loop(0, HT, combine, None)

    def finish(n, _):
        t = n // 2 + HT * lax.rem(n, 2)
        send_x(t).wait_recv()
        send_y(t).wait_recv()
        total = term(3, t) + rx[:, cols(t)].astype(f32) + ry[:, cols(t)].astype(f32)
        xr[:, cols(t)] = (xr[:, cols(t)].astype(f32) + total).astype(bf16)
        pltpu.make_async_copy(xr.at[:, cols(t)], o_ref.at[:, cols(t)], out_s.at[t]).start()

    lax.fori_loop(0, 2 * HT, finish, None)
    for t in range(2 * HT):
        send_x(t).wait_send()
        send_y(t).wait_send()
        (send_d if t < HT else send_e)(t).wait_send()
        pltpu.make_async_copy(xr.at[:, cols(t)], o_ref.at[:, cols(t)], out_s.at[t]).wait()
    for i in range(4):
        exchange(i).wait_send()


def solution(mesh):
    def step(x, gain, wq, wk, wv, wo):
        rate = THETA ** (-np.arange(HEAD // 2) / (HEAD // 2))
        near = np.arange(CH)[:, None] * rate
        far = (np.arange(SEQ // CH) * CH)[:, None] * rate
        near, far = (np.stack([np.cos(a), np.sin(a)]).astype(np.float32) for a in (near, far))
        hbm = pl.BlockSpec(memory_space=pl.ANY)
        dma, V = pltpu.SemaphoreType.DMA, pltpu.VMEM
        return pl.pallas_call(
            kernel,
            out_shape=jax.ShapeDtypeStruct((ROWS, D), bf16),
            in_specs=[hbm] * 8,
            out_specs=hbm,
            scratch_shapes=[
                V((ROWS, D), bf16),
                V((SEQ, D), bf16),
                V((3, D, WIDTH), bf16),
                V((2 * WIDTH, D), bf16),
                V((2, SEQ, HEAD), bf16),
                V((2, SEQ, HEAD), bf16),
                V((2, HEAD + SUMS, SEQ), bf16),
                V((4, ROWS, WIDTH), bf16),
                V((ROWS, D), bf16),
                V((ROWS, D), bf16),
                V((ROWS, D), bf16),
                V((8, STRIP), f32),
                V((2 * NS, HEAD + SUMS, STRIP), f32),
                V((D,), bf16), V(near.shape, f32), V(far.shape, f32),
                dma((8 + NCH,)), dma((3, NCH)), dma((3, NCH)), dma((5, NCH)), dma((5, NCH)), dma((2,)), dma((2, 4)),
                dma((3, 2 * HT)), dma((3, 2 * HT)), dma((2 * HT,)),
            ],
            compiler_params=pltpu.CompilerParams(collective_id=0, has_side_effects=True, vmem_limit_bytes=67043328),
        )(x, gain, wq, wk, wv, wo, near, far)

    tokens, columns = P(("dp", "tp"), None), P(None, "tp")
    return jax.shard_map(
        step,
        mesh=mesh,
        in_specs=(tokens, P(None), columns, columns, columns, P("tp", None)),
        out_specs=tokens,
        check_vma=False,
    )
```

```python
import functools

import jax
import jax.numpy as jnp
import numpy as np
from jax import lax
from jax.experimental import pallas as pl
from jax.experimental.pallas import tpu as pltpu
from jax.sharding import PartitionSpec as P

HEAD = 256
THETA = 10000
LOG2E = 1.4426950408889634
NEG = -1e30
EPS = 1e-6
CH = 128
NCH = 3
ROWS = CH * NCH
D = 3072
HALF = D // 2
TILE = 512
HT = HALF // TILE
SEQ = 8 * ROWS
CHIP = 2 * ROWS
STRIP = 256
NS = CHIP // STRIP
SUMS = 16
WIDTH = 2 * HEAD
SCALE = HEAD**-0.5
E2 = SCALE * LOG2E

f32, bf16 = jnp.float32, jnp.bfloat16


def dot(a, b, ca=1, cb=0):
    return lax.dot_general(a, b, (((ca,), (cb,)), ((), ())), preferred_element_type=f32)


def kernel(x_ref, gain_ref, wq_ref, wk_ref, wv_ref, wo_ref, near_ref, far_ref, o_ref,
           xr, xg, w, wo, q, k, vt, pb, rd, rx, ry, top_s, mix_s, gain_v, near_v, far_v,
           load, own_s, arr, fwd_s, arr2, wo_s, ex_s, rs_s, rs_r, out_s):
    me = lax.axis_index("tp")
    chip = me // 2
    core = me - 2 * chip
    chip_x = lax.rem(chip + 2, 4)
    chip_y = chip + 1 - 2 * lax.rem(chip, 2)
    chip_d = 3 - chip
    other, dev_x, dev_y = 2 * chip + 1 - core, 2 * chip_x + core, 2 * chip_y + core

    def remote(src, dst, s, r, to):
        return pltpu.make_async_remote_copy(src_ref=src, dst_ref=dst, send_sem=s, recv_sem=r, device_id={"tp": to},
                                            device_id_type=pl.DeviceIdType.MESH)

    lgain = pltpu.make_async_copy(gain_ref, gain_v, load.at[5])
    lgain.start()
    lxs = [pltpu.make_async_copy(x_ref.at[j * CH : (j + 1) * CH], xr.at[j * CH : (j + 1) * CH], load.at[8 + j]) for j in range(NCH)]
    for c in lxs:
        c.start()
    lnear, lfar = pltpu.make_async_copy(near_ref, near_v, load.at[6]), pltpu.make_async_copy(far_ref, far_v, load.at[7])
    lnear.start()
    lfar.start()
    lws = [pltpu.make_async_copy(r, w.at[i], load.at[1 + i]) for i, r in enumerate((wq_ref, wk_ref, wv_ref))]
    for c in lws:
        c.start()
    lwo = pltpu.make_async_copy(wo_ref, wo.at[0:WIDTH], load.at[4])
    lwo.start()

    barrier = pltpu.get_barrier_semaphore()
    for to in (other, dev_x, dev_y):
        pl.semaphore_signal(barrier, inc=1, device_id={"tp": to}, device_id_type=pl.DeviceIdType.MESH)
    lgain.wait()
    lxs[0].wait()

    def piece(p):
        return pl.ds(pl.multiple_of(p * CH, CH), CH)

    def nbr(j, i):
        return 2 * NCH + 4 * j + i

    def diag(j, i):
        return 6 * NCH + 2 * j + i

    def own_other(j):
        return remote(xg.at[piece(j)], xg.at[piece(NCH + j)], own_s.at[0, j], arr.at[0, j], other)

    def own_x(j):
        return remote(xg.at[piece(j)], xg.at[piece(nbr(j, 0))], own_s.at[1, j], arr.at[1, j], dev_x)

    def own_y(j):
        return remote(xg.at[piece(j)], xg.at[piece(nbr(j, 2))], own_s.at[2, j], arr.at[2, j], dev_y)

    def x_other(j):
        return remote(xg.at[piece(nbr(j, 0))], xg.at[piece(nbr(j, 1))], fwd_s.at[0, j], arr2.at[0, j], other)

    def y_other(j):
        return remote(xg.at[piece(nbr(j, 2))], xg.at[piece(nbr(j, 3))], fwd_s.at[1, j], arr2.at[1, j], other)

    def x_on(j):
        return remote(xg.at[piece(nbr(j, 0)), 0:HALF], xg.at[piece(diag(j, 0)), 0:HALF], fwd_s.at[2, j], arr2.at[2, j], dev_y)

    def y_on(j):
        return remote(xg.at[piece(nbr(j, 2)), HALF:D], xg.at[piece(diag(j, 0)), HALF:D], fwd_s.at[3, j], arr2.at[3, j], dev_x)

    def d_other(j):
        return remote(xg.at[piece(diag(j, 0))], xg.at[piece(diag(j, 1))], fwd_s.at[4, j], arr2.at[4, j], other)

    def pass_on(j):
        x_on(j).wait_recv()
        y_on(j).wait_recv()
        d_other(j).start()

    gain = gain_v[...].reshape(1, D).astype(f32)
    SUB = 32

    def norm(i, _):
        rows = pl.ds(pl.multiple_of(i * SUB, SUB), SUB)
        wide = xr[rows, :].astype(f32)
        scale = lax.rsqrt(jnp.mean(wide * wide, -1, keepdims=True) + EPS)
        xg[rows, :] = (wide * scale * gain).astype(bf16)

    per = CH // SUB
    lax.fori_loop(0, per, norm, None)
    pl.semaphore_wait(barrier, 3)
    for j in range(NCH):
        own_x(j).start()
        own_y(j).start()
        own_other(j).start()
        if j + 1 < NCH:
            lxs[j + 1].wait()
            lax.fori_loop((j + 1) * per, (j + 2) * per, norm, None)
    wo_copy = remote(wo_ref, wo.at[WIDTH : 2 * WIDTH], wo_s.at[0], wo_s.at[1], other)
    wo_copy.start()
    for h in range(2):
        vt[h, HEAD : HEAD + SUMS, :] = jnp.ones((SUMS, SEQ), bf16)
    for c in (*lws, lnear, lfar):
        c.wait()

    def chunk_of(p):
        mine, theirs = 2 * chip + core, 2 * chip + 1 - core
        n = jnp.maximum(p - 2 * NCH, 0)
        nj, ni = n // 4, lax.rem(n, 4)
        nd = 2 * jnp.where(ni < 2, chip_x, chip_y) + jnp.where(lax.rem(ni, 2) == 0, core, 1 - core)
        m = jnp.maximum(p - 6 * NCH, 0)
        mj, mi = m // 2, lax.rem(m, 2)
        md = 2 * chip_d + jnp.where(mi == 0, core, 1 - core)
        at = jnp.where(p < NCH, mine * NCH + p, theirs * NCH + p - NCH)
        at = jnp.where(p >= 2 * NCH, nd * NCH + nj, at)
        return jnp.where(p >= 6 * NCH, md * NCH + mj, at)

    def project(b):
        @pl.when(b == 1)
        def _():
            own_other(0).wait_recv()

        @pl.when(b == 2)
        def _():
            own_other(1).wait_recv()
            own_other(2).wait_recv()

        for j in range(NCH):

            @pl.when(b == NCH + 2 * j)
            def _():
                own_x(j).wait_recv()
                x_other(j).start()
                x_on(j).start()
                own_y(j).wait_recv()
                y_other(j).start()
                y_on(j).start()
                x_other(j).wait_recv()

            @pl.when(b == NCH + 2 * j + 1)
            def _():
                y_other(j).wait_recv()

            @pl.when(b == 3 * NCH + j)
            def _():
                if j < NCH - 1:
                    pass_on(j)
                d_other(j).wait_recv()

        rows = xg[pl.ds(pl.multiple_of(b * 2 * CH, 2 * CH), 2 * CH), :]
        places, trig = [], []
        for i in range(2):
            at = chunk_of(2 * b + i)
            places.append(pl.ds(pl.multiple_of(at * CH, CH), CH))
            cf, sf = far_v[0, pl.ds(at, 1), :], far_v[1, pl.ds(at, 1), :]
            cn, sn = near_v[0], near_v[1]
            trig.append((cf * cn - sf * sn, sf * cn + cf * sn))
        for n, to in ((0, q), (1, k)):
            for h in range(2):
                t = dot(rows, w[n, :, h * HEAD : (h + 1) * HEAD]).astype(bf16).astype(f32)
                for i in range(2):
                    a, b_ = t[i * CH : (i + 1) * CH, : HEAD // 2], t[i * CH : (i + 1) * CH, HEAD // 2 :]
                    cos, sin = trig[i]
                    to[h, places[i], :] = jnp.concatenate([a * cos - b_ * sin, b_ * cos + a * sin], -1).astype(bf16)
        for h in range(2):
            t = dot(rows, w[2, :, h * HEAD : (h + 1) * HEAD]).astype(bf16)
            for i in range(2):
                vt[h, 0:HEAD, places[i]] = t[i * CH : (i + 1) * CH].T

    def place(i):
        return pl.ds(pl.multiple_of(i * WIDTH, WIDTH), WIDTH)

    def attention(i, to, strips=range(NS)):
        pieces = [(h, s) for h in range(2) for s in strips]
        q0 = pl.multiple_of(to * CHIP, CHIP)
        for n in range(len(pieces)):
            top_s[n : n + 1, :] = jnp.full((1, STRIP), NEG, f32)
            mix_s[n] = jnp.zeros(mix_s.shape[1:], f32)

        def block(k0, masked):
            scores = []
            for h, s in pieces:
                keys = (s + 1) * STRIP if masked else CHIP
                qs = q[h, pl.ds(q0 + s * STRIP, STRIP), :]
                scores.append(dot(k[h, pl.ds(k0, keys), :], qs, 1, 1))
            weights, keeps = [], []
            for n, ((h, s), sc) in enumerate(zip(pieces, scores)):
                if masked:
                    ok = (lax.broadcasted_iota(jnp.int32, sc.shape, 0) - s * STRIP) <= lax.broadcasted_iota(jnp.int32, sc.shape, 1)
                    sc = jnp.where(ok, sc, 2 * NEG)
                old = top_s[n : n + 1, :]
                top = jnp.maximum(old, sc.max(axis=0, keepdims=True))
                top_s[n : n + 1, :] = top
                weights.append(jnp.exp2((sc - top) * E2).astype(bf16))
                keeps.append(jnp.exp2((old - top) * E2))
            for n, (h, s) in enumerate(pieces):
                keys = (s + 1) * STRIP if masked else CHIP
                mix_s[n] = mix_s[n] * keeps[n] + dot(vt[h, :, pl.ds(k0, keys)], weights[n])

        lax.fori_loop(0, to, lambda j, _: block(pl.multiple_of(j * CHIP, CHIP), False), None)
        block(q0, True)
        for n, (h, s) in enumerate(pieces):
            out = mix_s[n, 0:HEAD, :] * (1 / mix_s[n, HEAD : HEAD + 1, :])
            xg[s * STRIP : (s + 1) * STRIP, pl.ds(pl.multiple_of(i * WIDTH + h * HEAD, HEAD), HEAD)] = out.T.astype(bf16)

    PARTS = (slice(0, STRIP), slice(STRIP, ROWS))
    WHOLE = slice(0, ROWS)

    def results(of, part=WHOLE):
        return pl.ds(pl.multiple_of(of * ROWS + part.start, CH), part.stop - part.start)

    def exchange(i, part=WHOLE, slot=None):
        slot = i if slot is None else slot
        return remote(xg.at[results(1 - core, part), place(i)], pb.at[i, part], ex_s.at[0, slot], ex_s.at[1, slot], other)

    def term(i, t, part=WHOLE):
        mine = xg[results(core, part), place(i)]
        cols = pl.ds(pl.multiple_of(t * TILE, TILE), TILE)
        return dot(jnp.concatenate([mine, pb[i, part]], axis=1), wo[:, cols])

    def cols(t):
        return pl.ds(pl.multiple_of(t * TILE, TILE), TILE)

    SX, SY, SD = (slice(n * ROWS, (n + 1) * ROWS) for n in range(2, 5))

    def send_x(t):
        return remote(xg.at[SX, cols(t)], rx.at[:, cols(t)], rs_s.at[0, t], rs_r.at[0, t], dev_x)

    def send_y(t):
        return remote(xg.at[SY, cols(t)], ry.at[:, cols(t)], rs_s.at[1, t], rs_r.at[1, t], dev_y)

    def send_yd(u):
        rows, at = pl.ds(pl.multiple_of(u // 2 * ROWS, ROWS), ROWS), cols(4 + lax.rem(u, 2))
        return remote(xg.at[rows, at], ry.at[:, cols(HT + u)], rs_s.at[1, HT + u], rs_r.at[1, HT + u], dev_y)

    def send_d(t, p):
        rows = slice(SD.start + PARTS[p].start, SD.start + PARTS[p].stop)
        return remote(xg.at[rows, cols(t)], rd.at[PARTS[p], cols(t)], rs_s.at[2 + p, t], rs_r.at[2 + p, t], dev_x)

    def send_e(t, p):
        rows = slice(SD.start + PARTS[p].start, SD.start + PARTS[p].stop)
        return remote(xg.at[rows, cols(t)], rd.at[PARTS[p], cols(t)], rs_s.at[2 + p, t], rs_r.at[2 + p, t], dev_y)

    def diagonal(p):
        rows = slice(SD.start + PARTS[p].start, SD.start + PARTS[p].stop)

        def one(t, _):
            xg[rows, cols(t)] = term(2, t, PARTS[p]).astype(bf16)
            send_d(t, p).start()
            xg[rows, cols(HT + t)] = term(2, HT + t, PARTS[p]).astype(bf16)
            send_e(HT + t, p).start()

        lax.fori_loop(0, HT, one, None)

    def item(n):
        x_first = chip_x < chip_y
        to = jnp.where(n == 2, chip, jnp.where((n == 0) == x_first, chip_x, chip_y))
        i = jnp.where(n == 2, 3, jnp.where((n == 0) == x_first, 0, 1))
        attention(i, to)
        ex = exchange(i)
        ex.start()

        @pl.when(n == 0)
        def _():
            for c in (x_other, y_other, x_on, y_on):
                c(0).wait_send()

        ex.wait_recv()

        def direct(t, _):
            tx, ty = t, HT + t

            @pl.when(i == 0)
            def _():
                xg[SX, cols(tx)] = term(0, tx).astype(bf16)
                send_x(tx).start()

            @pl.when(i == 1)
            def _():
                xg[pl.ds(pl.multiple_of(t // 2 * ROWS, ROWS), ROWS), cols(4 + lax.rem(t, 2))] = term(1, ty).astype(bf16)
                send_yd(t).start()

        lax.fori_loop(0, jnp.where(i == 3, 0, HT), direct, None)

    early = jnp.where(chip == 0, 2, jnp.where(chip == 3, 0, 1))
    first = 3 * NCH
    late = first + NCH + 2

    def step(n, _):
        @pl.when(n == first)
        def _():
            lwo.wait()
            wo_copy.wait()
            for j in range(NCH):
                for c in (own_other, own_x, own_y):
                    c(j).wait_send()

        m = n - early
        is_item = ((n >= first) & (n < first + early)) | (m >= late)
        on = (n < first) | (m >= first)

        @pl.when((n < first) | ((m >= first) & (m < first + 2)) | (m == first + 3))
        def _():
            project(jnp.where(n < first, n, jnp.where(m == first + 3, first + 2, m)))

        @pl.when(on & (m == first + 2) & (n >= first))
        def _():
            attention(2, chip_d, range(1))

            @pl.when(core == 1)
            def _():
                exchange(2, PARTS[0]).start()

            pass_on(NCH - 1)
            for j in range(1, NCH):
                for c in (x_other, y_other, x_on, y_on):
                    c(j).wait_send()

            @pl.when(core == 0)
            def _():
                exchange(2, PARTS[0]).wait_recv()
                diagonal(0)

        @pl.when(on & (m == first + 4) & (n >= first))
        def _():
            for j in range(NCH):
                d_other(j).wait_send()
            attention(2, chip_d, range(1, NS))

            @pl.when(core == 0)
            def _():
                exchange(2, PARTS[0]).start()

            exchange(2, PARTS[1], 4).start()

            @pl.when(core == 1)
            def _():
                exchange(2, PARTS[0]).wait_recv()
                diagonal(0)

            exchange(2, PARTS[1], 4).wait_recv()
            diagonal(1)

        @pl.when(is_item)
        def _():
            item(jnp.where(n < first + early, n - first, m - late + early))

    lax.fori_loop(0, late + 3, step, None)

    def combine(t, _):
        tx, ty = HT + t, t
        send_e(tx, 0).wait_recv()
        send_e(tx, 1).wait_recv()
        xg[SX, cols(tx)] = (term(0, tx) + rd[:, cols(tx)].astype(f32)).astype(bf16)
        send_x(tx).start()
        send_d(ty, 0).wait_recv()
        send_d(ty, 1).wait_recv()
        xg[SY, cols(ty)] = (term(1, ty) + rd[:, cols(ty)].astype(f32)).astype(bf16)
        send_y(ty).start()

    lax.fori_loop(0, HT, combine, None)

    def finish(n, _):
        t = n // 2 + HT * lax.rem(n, 2)
        send_x(t).wait_recv()
        send_y(t).wait_recv()
        total = term(3, t) + rx[:, cols(t)].astype(f32) + ry[:, cols(t)].astype(f32)
        xr[:, cols(t)] = (xr[:, cols(t)].astype(f32) + total).astype(bf16)
        pltpu.make_async_copy(xr.at[:, cols(t)], o_ref.at[:, cols(t)], out_s.at[t]).start()

    lax.fori_loop(0, 2 * HT, finish, None)
    for t in range(2 * HT):
        send_x(t).wait_send()
        send_y(t).wait_send()
        for p in range(2):
            (send_d if t < HT else send_e)(t, p).wait_send()
        pltpu.make_async_copy(xr.at[:, cols(t)], o_ref.at[:, cols(t)], out_s.at[t]).wait()
    for i in (0, 1, 3):
        exchange(i).wait_send()
    exchange(2, PARTS[0]).wait_send()
    exchange(2, PARTS[1], 4).wait_send()


def solution(mesh):
    def step(x, gain, wq, wk, wv, wo):
        rate = THETA ** (-np.arange(HEAD // 2) / (HEAD // 2))
        near = np.arange(CH)[:, None] * rate
        far = (np.arange(SEQ // CH) * CH)[:, None] * rate
        near, far = (np.stack([np.cos(a), np.sin(a)]).astype(np.float32) for a in (near, far))
        hbm = pl.BlockSpec(memory_space=pl.ANY)
        dma, V = pltpu.SemaphoreType.DMA, pltpu.VMEM
        return pl.pallas_call(
            kernel,
            out_shape=jax.ShapeDtypeStruct((ROWS, D), bf16),
            in_specs=[hbm] * 8,
            out_specs=hbm,
            scratch_shapes=[
                V((ROWS, D), bf16),
                V((SEQ, D), bf16),
                V((3, D, WIDTH), bf16),
                V((2 * WIDTH, D), bf16),
                V((2, SEQ, HEAD), bf16),
                V((2, SEQ, HEAD), bf16),
                V((2, HEAD + SUMS, SEQ), bf16),
                V((4, ROWS, WIDTH), bf16),
                V((ROWS, D), bf16),
                V((ROWS, D), bf16),
                V((ROWS, D), bf16),
                V((8, STRIP), f32),
                V((2 * NS, HEAD + SUMS, STRIP), f32),
                V((D,), bf16), V(near.shape, f32), V(far.shape, f32),
                dma((8 + NCH,)), dma((3, NCH)), dma((3, NCH)), dma((5, NCH)), dma((5, NCH)), dma((2,)), dma((2, 5)),
                dma((4, 2 * HT)), dma((4, 2 * HT)), dma((2 * HT,)),
            ],
            compiler_params=pltpu.CompilerParams(collective_id=0, has_side_effects=True, vmem_limit_bytes=67043328),
        )(x, gain, wq, wk, wv, wo, near, far)

    tokens, columns = P(("dp", "tp"), None), P(None, "tp")
    return jax.shard_map(
        step,
        mesh=mesh,
        in_specs=(tokens, P(None), columns, columns, columns, P("tp", None)),
        out_specs=tokens,
        check_vma=False,
    )
```

```python
import functools

import jax
import jax.numpy as jnp
import numpy as np
from jax import lax
from jax.experimental import pallas as pl
from jax.experimental.pallas import tpu as pltpu
from jax.sharding import PartitionSpec as P

HEAD = 256
THETA = 10000
LOG2E = 1.4426950408889634
NEG = -1e30
EPS = 1e-6
CH = 128
NCH = 3
ROWS = CH * NCH
D = 3072
HALF = D // 2
TILE = 512
HT = HALF // TILE
SEQ = 8 * ROWS
CHIP = 2 * ROWS
STRIP = 256
NS = CHIP // STRIP
SUMS = 16
WIDTH = 2 * HEAD
SCALE = HEAD**-0.5
E2 = SCALE * LOG2E

f32, bf16 = jnp.float32, jnp.bfloat16


def dot(a, b, ca=1, cb=0):
    return lax.dot_general(a, b, (((ca,), (cb,)), ((), ())), preferred_element_type=f32)


def kernel(x_ref, gain_ref, wq_ref, wk_ref, wv_ref, wo_ref, near_ref, far_ref, o_ref, diag_h, direct_h,
           xg, w, wo, q, k, vt, pb, top_s, mix_s, gain_v, near_v, far_v,
           load, own_s, arr, fwd_s, arr2, wo_s, ex_s, rs_s, rs_r, fetch, free):
    me = lax.axis_index("tp")
    chip = me // 2
    core = me - 2 * chip
    chip_x = lax.rem(chip + 2, 4)
    chip_y = chip + 1 - 2 * lax.rem(chip, 2)
    chip_d = 3 - chip
    other, dev_x, dev_y = 2 * chip + 1 - core, 2 * chip_x + core, 2 * chip_y + core

    def remote(src, dst, s, r, to):
        return pltpu.make_async_remote_copy(src_ref=src, dst_ref=dst, send_sem=s, recv_sem=r, device_id={"tp": to},
                                            device_id_type=pl.DeviceIdType.MESH)

    def piece(p):
        return pl.ds(pl.multiple_of(p * CH, CH), CH)

    lgain = pltpu.make_async_copy(gain_ref, gain_v, load.at[5])
    lgain.start()
    lxs = [pltpu.make_async_copy(x_ref.at[piece(j)], vt.at[j // 2, j % 2 * CH : (j % 2 + 1) * CH], load.at[8 + j]) for j in range(NCH)]
    for c in lxs:
        c.start()
    lnear, lfar = pltpu.make_async_copy(near_ref, near_v, load.at[6]), pltpu.make_async_copy(far_ref, far_v, load.at[7])
    lnear.start()
    lfar.start()
    lws = [pltpu.make_async_copy(r, w.at[i], load.at[1 + i]) for i, r in enumerate((wq_ref, wk_ref, wv_ref))]
    for c in lws:
        c.start()
    lwo = pltpu.make_async_copy(wo_ref, wo.at[0:WIDTH], load.at[4])
    lwo.start()

    barrier = pltpu.get_barrier_semaphore()
    for to in (other, dev_x, dev_y):
        pl.semaphore_signal(barrier, inc=1, device_id={"tp": to}, device_id_type=pl.DeviceIdType.MESH)
    lgain.wait()
    lxs[0].wait()

    def nbr(j, i):
        return 2 * NCH + 4 * j + i

    def diag(j, i):
        return 6 * NCH + 2 * j + i

    def own_other(j):
        return remote(xg.at[piece(j)], xg.at[piece(NCH + j)], own_s.at[0, j], arr.at[0, j], other)

    def own_x(j):
        return remote(xg.at[piece(j)], xg.at[piece(nbr(j, 0))], own_s.at[1, j], arr.at[1, j], dev_x)

    def own_y(j):
        return remote(xg.at[piece(j)], xg.at[piece(nbr(j, 2))], own_s.at[2, j], arr.at[2, j], dev_y)

    def x_other(j):
        return remote(xg.at[piece(nbr(j, 0))], xg.at[piece(nbr(j, 1))], fwd_s.at[0, j], arr2.at[0, j], other)

    def y_other(j):
        return remote(xg.at[piece(nbr(j, 2))], xg.at[piece(nbr(j, 3))], fwd_s.at[1, j], arr2.at[1, j], other)

    def x_on(j):
        return remote(xg.at[piece(nbr(j, 0)), 0:HALF], xg.at[piece(diag(j, 0)), 0:HALF], fwd_s.at[2, j], arr2.at[2, j], dev_y)

    def y_on(j):
        return remote(xg.at[piece(nbr(j, 2)), HALF:D], xg.at[piece(diag(j, 0)), HALF:D], fwd_s.at[3, j], arr2.at[3, j], dev_x)

    def d_other(j):
        return remote(xg.at[piece(diag(j, 0))], xg.at[piece(diag(j, 1))], fwd_s.at[4, j], arr2.at[4, j], other)

    def pass_on(j):
        x_on(j).wait_recv()
        y_on(j).wait_recv()
        d_other(j).start()

    gain = gain_v[...].reshape(1, D).astype(f32)
    SUB = 32
    per = CH // SUB

    def norm(i, _):
        rows = pl.ds(pl.multiple_of(i * SUB, SUB), SUB)
        p = i // per
        wide = vt[p // 2, pl.ds(pl.multiple_of(lax.rem(p, 2) * CH + lax.rem(i, per) * SUB, SUB), SUB), :].astype(f32)
        scale = lax.rsqrt(jnp.mean(wide * wide, -1, keepdims=True) + EPS)
        xg[rows, :] = (wide * scale * gain).astype(bf16)

    lax.fori_loop(0, per, norm, None)
    pl.semaphore_wait(barrier, 3)
    for j in range(NCH):
        own_x(j).start()
        own_y(j).start()
        own_other(j).start()
        if j + 1 < NCH:
            lxs[j + 1].wait()
            lax.fori_loop((j + 1) * per, (j + 2) * per, norm, None)
    wo_copy = remote(wo_ref, wo.at[WIDTH : 2 * WIDTH], wo_s.at[0], wo_s.at[1], other)
    wo_copy.start()
    for h in range(2):
        vt[h, HEAD : HEAD + SUMS, :] = jnp.ones((SUMS, SEQ), bf16)
    for c in (*lws, lnear, lfar):
        c.wait()

    def chunk_of(p):
        mine, theirs = 2 * chip + core, 2 * chip + 1 - core
        n = jnp.maximum(p - 2 * NCH, 0)
        nj, ni = n // 4, lax.rem(n, 4)
        nd = 2 * jnp.where(ni < 2, chip_x, chip_y) + jnp.where(lax.rem(ni, 2) == 0, core, 1 - core)
        m = jnp.maximum(p - 6 * NCH, 0)
        mj, mi = m // 2, lax.rem(m, 2)
        md = 2 * chip_d + jnp.where(mi == 0, core, 1 - core)
        at = jnp.where(p < NCH, mine * NCH + p, theirs * NCH + p - NCH)
        at = jnp.where(p >= 2 * NCH, nd * NCH + nj, at)
        return jnp.where(p >= 6 * NCH, md * NCH + mj, at)

    def project(b):
        @pl.when(b == 1)
        def _():
            own_other(0).wait_recv()

        @pl.when(b == 2)
        def _():
            own_other(1).wait_recv()
            own_other(2).wait_recv()

        for j in range(NCH):

            @pl.when(b == NCH + 2 * j)
            def _():
                own_x(j).wait_recv()
                x_other(j).start()
                x_on(j).start()
                own_y(j).wait_recv()
                y_other(j).start()
                y_on(j).start()
                x_other(j).wait_recv()

            @pl.when(b == NCH + 2 * j + 1)
            def _():
                y_other(j).wait_recv()

            @pl.when(b == 3 * NCH + j)
            def _():
                if j < NCH - 1:
                    pass_on(j)
                d_other(j).wait_recv()

        rows = xg[pl.ds(pl.multiple_of(b * 2 * CH, 2 * CH), 2 * CH), :]
        places, trig = [], []
        for i in range(2):
            at = chunk_of(2 * b + i)
            places.append(pl.ds(pl.multiple_of(at * CH, CH), CH))
            cf, sf = far_v[0, pl.ds(at, 1), :], far_v[1, pl.ds(at, 1), :]
            cn, sn = near_v[0], near_v[1]
            trig.append((cf * cn - sf * sn, sf * cn + cf * sn))
        for n, to in ((0, q), (1, k)):
            for h in range(2):
                t = dot(rows, w[n, :, h * HEAD : (h + 1) * HEAD]).astype(bf16).astype(f32)
                for i in range(2):
                    a, b_ = t[i * CH : (i + 1) * CH, : HEAD // 2], t[i * CH : (i + 1) * CH, HEAD // 2 :]
                    cos, sin = trig[i]
                    to[h, places[i], :] = jnp.concatenate([a * cos - b_ * sin, b_ * cos + a * sin], -1).astype(bf16)
        for h in range(2):
            t = dot(rows, w[2, :, h * HEAD : (h + 1) * HEAD]).astype(bf16)
            for i in range(2):
                vt[h, 0:HEAD, places[i]] = t[i * CH : (i + 1) * CH].T

    def place(i):
        return pl.ds(pl.multiple_of(i * WIDTH, WIDTH), WIDTH)

    def attention(i, to, strips=range(NS)):
        if len(strips) == NS:
            for h in range(2):
                attend(i, to, [(h, s) for s in strips])
        else:
            attend(i, to, [(h, s) for h in range(2) for s in strips])

    def attend(i, to, pieces):
        q0 = pl.multiple_of(to * CHIP, CHIP)
        for n in range(len(pieces)):
            top_s[n : n + 1, :] = jnp.full((1, STRIP), NEG, f32)
            mix_s[n] = jnp.zeros(mix_s.shape[1:], f32)

        def block(k0, masked):
            scores = []
            for h, s in pieces:
                keys = (s + 1) * STRIP if masked else CHIP
                qs = q[h, pl.ds(q0 + s * STRIP, STRIP), :]
                scores.append(dot(k[h, pl.ds(k0, keys), :], qs, 1, 1))
            weights, keeps = [], []
            for n, ((h, s), sc) in enumerate(zip(pieces, scores)):
                if masked:
                    ok = (lax.broadcasted_iota(jnp.int32, sc.shape, 0) - s * STRIP) <= lax.broadcasted_iota(jnp.int32, sc.shape, 1)
                    sc = jnp.where(ok, sc, 2 * NEG)
                old = top_s[n : n + 1, :]
                top = jnp.maximum(old, sc.max(axis=0, keepdims=True))
                top_s[n : n + 1, :] = top
                weights.append(jnp.exp2((sc - top) * E2).astype(bf16))
                keeps.append(jnp.exp2((old - top) * E2))
            for n, (h, s) in enumerate(pieces):
                keys = (s + 1) * STRIP if masked else CHIP
                mix_s[n] = mix_s[n] * keeps[n] + dot(vt[h, :, pl.ds(k0, keys)], weights[n])

        lax.fori_loop(0, to, lambda j, _: block(pl.multiple_of(j * CHIP, CHIP), False), None)
        block(q0, True)
        for n, (h, s) in enumerate(pieces):
            out = mix_s[n, 0:HEAD, :] * (1 / mix_s[n, HEAD : HEAD + 1, :])
            xg[s * STRIP : (s + 1) * STRIP, pl.ds(pl.multiple_of(i * WIDTH + h * HEAD, HEAD), HEAD)] = out.T.astype(bf16)

    PARTS = (slice(0, STRIP), slice(STRIP, ROWS))
    WHOLE = slice(0, ROWS)

    def results(of, part=WHOLE):
        return pl.ds(pl.multiple_of(of * ROWS + part.start, CH), part.stop - part.start)

    def exchange(i, part=WHOLE, slot=None):
        slot = i if slot is None else slot
        return remote(xg.at[results(1 - core, part), place(i)], pb.at[i, part], ex_s.at[0, slot], ex_s.at[1, slot], other)

    def term(i, t, part=WHOLE):
        mine = xg[results(core, part), place(i)]
        cols = pl.ds(pl.multiple_of(t * TILE, TILE), TILE)
        return dot(jnp.concatenate([mine, pb[i, part]], axis=1), wo[:, cols])

    def cols(t):
        return pl.ds(pl.multiple_of(t * TILE, TILE), TILE)

    SX, SY, SD = (slice(n * ROWS, (n + 1) * ROWS) for n in range(2, 5))
    SUMS_IN = slice(5 * ROWS, 6 * ROWS)
    RD, DIR = (slice(n * ROWS, (n + 1) * ROWS) for n in range(6, 8))
    lxr = pltpu.make_async_copy(x_ref, o_ref, load.at[0])

    def send_xd(t):
        return remote(xg.at[SX, cols(t)], direct_h.at[:, cols(t)], rs_s.at[0, t], rs_r.at[0, t], dev_x)

    def send_yd(t):
        rows, at = pl.ds(pl.multiple_of(t // 2 * ROWS, ROWS), ROWS), cols(4 + lax.rem(t, 2))
        return remote(xg.at[rows, at], direct_h.at[:, cols(HT + t)], rs_s.at[1, HT + t], rs_r.at[1, HT + t], dev_y)

    def send_x(t):
        return remote(xg.at[SX, cols(HT + t)], xg.at[SUMS_IN, cols(HT + t)], rs_s.at[0, HT + t], rs_r.at[0, HT + t], dev_x)

    def send_y(t):
        return remote(xg.at[SY, cols(t)], xg.at[SUMS_IN, cols(t)], rs_s.at[1, t], rs_r.at[1, t], dev_y)

    def fetch_d(t):
        return pltpu.make_async_copy(diag_h.at[:, cols(t)], xg.at[RD, cols(t)], fetch.at[0, t])

    def fetch_direct(t):
        return pltpu.make_async_copy(direct_h.at[:, cols(t)], xg.at[DIR, cols(t)], fetch.at[1, t])

    def send_d(t, p):
        rows = slice(SD.start + PARTS[p].start, SD.start + PARTS[p].stop)
        return remote(xg.at[rows, cols(t)], diag_h.at[PARTS[p], cols(t)], rs_s.at[2 + p, t], rs_r.at[2 + p, t], dev_x)

    def send_e(t, p):
        rows = slice(SD.start + PARTS[p].start, SD.start + PARTS[p].stop)
        return remote(xg.at[rows, cols(t)], diag_h.at[PARTS[p], cols(t)], rs_s.at[2 + p, t], rs_r.at[2 + p, t], dev_y)

    def diagonal(p):
        rows = slice(SD.start + PARTS[p].start, SD.start + PARTS[p].stop)

        def one(t, _):
            xg[rows, cols(t)] = term(2, t, PARTS[p]).astype(bf16)
            send_d(t, p).start()
            xg[rows, cols(HT + t)] = term(2, HT + t, PARTS[p]).astype(bf16)
            send_e(HT + t, p).start()

        lax.fori_loop(0, HT, one, None)

    def item(n):
        x_first = chip_x < chip_y
        to = jnp.where(n == 2, chip, jnp.where((n == 0) == x_first, chip_x, chip_y))
        i = jnp.where(n == 2, 3, jnp.where((n == 0) == x_first, 0, 1))
        attention(i, to)
        ex = exchange(i)
        ex.start()

        @pl.when(n == 0)
        def _():
            for c in (x_other, y_other, x_on, y_on):
                c(0).wait_send()

        ex.wait_recv()

        def direct(t, _):
            tx, ty = t, HT + t

            @pl.when(i == 0)
            def _():
                xg[SX, cols(tx)] = term(0, tx).astype(bf16)
                send_xd(t).start()

            @pl.when(i == 1)
            def _():
                xg[pl.ds(pl.multiple_of(t // 2 * ROWS, ROWS), ROWS), cols(4 + lax.rem(t, 2))] = term(1, ty).astype(bf16)
                send_yd(t).start()

        lax.fori_loop(0, jnp.where(i == 3, 0, HT), direct, None)

    early = jnp.where(chip == 0, 2, jnp.where(chip == 3, 0, 1))
    first = 3 * NCH
    late = first + NCH + 2

    def step(n, _):
        @pl.when(n == first)
        def _():
            lwo.wait()
            wo_copy.wait()
            for j in range(NCH):
                for c in (own_other, own_x, own_y):
                    c(j).wait_send()

        m = n - early
        is_item = ((n >= first) & (n < first + early)) | (m >= late)
        on = (n < first) | (m >= first)

        @pl.when((n < first) | ((m >= first) & (m < first + 2)) | (m == first + 3))
        def _():
            project(jnp.where(n < first, n, jnp.where(m == first + 3, first + 2, m)))

        @pl.when(on & (m == first + 2) & (n >= first))
        def _():
            attention(2, chip_d, range(1))

            @pl.when(core == 1)
            def _():
                exchange(2, PARTS[0]).start()

            pass_on(NCH - 1)
            for j in range(1, NCH):
                for c in (x_other, y_other, x_on, y_on):
                    c(j).wait_send()
            lxr.start()

            @pl.when(core == 0)
            def _():
                exchange(2, PARTS[0]).wait_recv()
                diagonal(0)

        @pl.when(on & (m == first + 4) & (n >= first))
        def _():
            for to in (dev_x, dev_y):
                pl.semaphore_signal(free, inc=1, device_id={"tp": to}, device_id_type=pl.DeviceIdType.MESH)
            for j in range(NCH):
                d_other(j).wait_send()
            attention(2, chip_d, range(1, NS))

            @pl.when(core == 0)
            def _():
                exchange(2, PARTS[0]).start()

            exchange(2, PARTS[1], 4).start()

            @pl.when(core == 1)
            def _():
                exchange(2, PARTS[0]).wait_recv()
                diagonal(0)

            exchange(2, PARTS[1], 4).wait_recv()
            diagonal(1)

        @pl.when(is_item)
        def _():
            item(jnp.where(n < first + early, n - first, m - late + early))

    lax.fori_loop(0, late + 3, step, None)

    def combine(t, _):
        tx, ty = HT + t, t
        send_e(tx, 0).wait_recv()
        send_e(tx, 1).wait_recv()
        fetch_d(tx).start()
        fetch_d(tx).wait()
        xg[SX, cols(tx)] = (term(0, tx) + xg[RD, cols(tx)].astype(f32)).astype(bf16)
        send_x(t).start()
        send_d(ty, 0).wait_recv()
        send_d(ty, 1).wait_recv()
        fetch_d(ty).start()
        fetch_d(ty).wait()
        xg[SY, cols(ty)] = (term(1, ty) + xg[RD, cols(ty)].astype(f32)).astype(bf16)
        send_y(t).start()

    pl.semaphore_wait(free, 2)
    lax.fori_loop(0, HT, combine, None)

    for t in range(HT):
        send_xd(t).wait_recv()
        fetch_direct(t).start()
        send_yd(t).wait_recv()
        fetch_direct(HT + t).start()
    lxr.wait()
    for t in range(2 * HT):
        fetch_direct(t).wait()

    def finish(t, _):
        def one(t):
            total = term(3, t) + xg[DIR, cols(t)].astype(f32) + xg[SUMS_IN, cols(t)].astype(f32)
            o_ref[:, cols(t)] = (o_ref[:, cols(t)].astype(f32) + total).astype(bf16)

        send_y(t).wait_recv()
        one(t)
        send_x(t).wait_recv()
        one(HT + t)

    lax.fori_loop(0, HT, finish, None)
    for t in range(HT):
        for c in (send_xd, send_yd, send_x, send_y):
            c(t).wait_send()
        for p in range(2):
            send_d(t, p).wait_send()
            send_e(HT + t, p).wait_send()
    for i in (0, 1, 3):
        exchange(i).wait_send()
    exchange(2, PARTS[0]).wait_send()
    exchange(2, PARTS[1], 4).wait_send()


def in_hbm(a):
    return pltpu.with_memory_space_constraint(jnp.asarray(a), pltpu.HBM)


def solution(mesh):
    def step(x, gain, wq, wk, wv, wo):
        rate = THETA ** (-np.arange(HEAD // 2) / (HEAD // 2))
        near = np.arange(CH)[:, None] * rate
        far = (np.arange(SEQ // CH) * CH)[:, None] * rate
        near, far = (np.stack([np.cos(a), np.sin(a)]).astype(np.float32) for a in (near, far))
        hbm = pl.BlockSpec(memory_space=pltpu.HBM)
        dma, V = pltpu.SemaphoreType.DMA, pltpu.VMEM
        return pl.pallas_call(
            kernel,
            out_shape=[jax.ShapeDtypeStruct((ROWS, D), bf16)] * 3,
            in_specs=[hbm] * 8,
            out_specs=[pl.BlockSpec(memory_space=pltpu.VMEM), hbm, hbm],
            scratch_shapes=[
                V((SEQ, D), bf16),
                V((3, D, WIDTH), bf16),
                V((2 * WIDTH, D), bf16),
                V((2, SEQ, HEAD), bf16),
                V((2, SEQ, HEAD), bf16),
                V((2, HEAD + SUMS, SEQ), bf16),
                V((4, ROWS, WIDTH), bf16),
                V((8, STRIP), f32),
                V((2 * NS - 2, HEAD + SUMS, STRIP), f32),
                V((D,), bf16), V(near.shape, f32), V(far.shape, f32),
                dma((8 + NCH,)), dma((3, NCH)), dma((3, NCH)), dma((5, NCH)), dma((5, NCH)), dma((2,)), dma((2, 5)),
                dma((4, 2 * HT)), dma((4, 2 * HT)), dma((2, 2 * HT)), pltpu.SemaphoreType.REGULAR,
            ],
            compiler_params=pltpu.CompilerParams(collective_id=0, has_side_effects=True, vmem_limit_bytes=51 * 2**20),
        )(x, in_hbm(gain), wq, wk, wv, wo, in_hbm(near), in_hbm(far))[0]

    tokens, columns = P(("dp", "tp"), None), P(None, "tp")
    return jax.shard_map(
        step,
        mesh=mesh,
        in_specs=(tokens, P(None), columns, columns, columns, P("tp", None)),
        out_specs=tokens,
        check_vma=False,
    )
```

```python
import functools

import jax
import jax.numpy as jnp
import numpy as np
from jax import lax
from jax.experimental import pallas as pl
from jax.experimental.pallas import tpu as pltpu
from jax.sharding import PartitionSpec as P

HEAD = 256
THETA = 10000
LOG2E = 1.4426950408889634
NEG = -1e30
EPS = 1e-6
CH = 128
NCH = 3
ROWS = CH * NCH
D = 3072
HALF = D // 2
TILE = 512
HT = HALF // TILE
SEQ = 8 * ROWS
CHIP = 2 * ROWS
STRIP = 256
NS = CHIP // STRIP
AHEAD = 3
SUMS = 8
WIDTH = 2 * HEAD
SCALE = HEAD**-0.5
E2 = SCALE * LOG2E

f32, bf16 = jnp.float32, jnp.bfloat16


def dot(a, b, ca=1, cb=0):
    return lax.dot_general(a, b, (((ca,), (cb,)), ((), ())), preferred_element_type=f32)


def kernel(x_ref, gain_ref, wq_ref, wk_ref, wv_ref, wo_ref, near_ref, far_ref, o_ref, diag_h, direct_h,
           xg, w, wo, q, k, vt, pb, top_s, mix_s, gain_v, near_v, far_v,
           load, own_s, arr, fwd_s, arr2, wo_s, ex_s, rs_s, rs_r, fetch, free):
    me = lax.axis_index("tp")
    chip = me // 2
    core = me - 2 * chip
    chip_x = lax.rem(chip + 2, 4)
    chip_y = chip + 1 - 2 * lax.rem(chip, 2)
    chip_d = 3 - chip
    other, dev_x, dev_y = 2 * chip + 1 - core, 2 * chip_x + core, 2 * chip_y + core

    def remote(src, dst, s, r, to):
        return pltpu.make_async_remote_copy(src_ref=src, dst_ref=dst, send_sem=s, recv_sem=r, device_id={"tp": to},
                                            device_id_type=pl.DeviceIdType.MESH)

    def piece(p):
        return pl.ds(pl.multiple_of(p * CH, CH), CH)

    lgain = pltpu.make_async_copy(gain_ref, gain_v, load.at[5])
    lgain.start()
    lxs = [pltpu.make_async_copy(x_ref.at[piece(j)], vt.at[j // 2, j % 2 * CH : (j % 2 + 1) * CH], load.at[8 + j]) for j in range(NCH)]
    for c in lxs:
        c.start()
    lnear, lfar = pltpu.make_async_copy(near_ref, near_v, load.at[6]), pltpu.make_async_copy(far_ref, far_v, load.at[7])
    lnear.start()
    lfar.start()
    lws = [pltpu.make_async_copy(r, w.at[i], load.at[1 + i]) for i, r in enumerate((wq_ref, wk_ref, wv_ref))]
    for c in lws:
        c.start()
    lwo = pltpu.make_async_copy(wo_ref, wo.at[0:WIDTH], load.at[4])
    lwo.start()

    barrier = pltpu.get_barrier_semaphore()
    for to in (other, dev_x, dev_y):
        pl.semaphore_signal(barrier, inc=1, device_id={"tp": to}, device_id_type=pl.DeviceIdType.MESH)
    lgain.wait()
    lxs[0].wait()

    def nbr(j, i):
        return 2 * NCH + 4 * j + i

    def diag(j, i):
        return 6 * NCH + 2 * j + i

    def own_other(j):
        return remote(xg.at[piece(j)], xg.at[piece(NCH + j)], own_s.at[0, j], arr.at[0, j], other)

    def own_x(j):
        return remote(xg.at[piece(j)], xg.at[piece(nbr(j, 0))], own_s.at[1, j], arr.at[1, j], dev_x)

    def own_y(j):
        return remote(xg.at[piece(j)], xg.at[piece(nbr(j, 2))], own_s.at[2, j], arr.at[2, j], dev_y)

    def x_other(j):
        return remote(xg.at[piece(nbr(j, 0))], xg.at[piece(nbr(j, 1))], fwd_s.at[0, j], arr2.at[0, j], other)

    def y_other(j):
        return remote(xg.at[piece(nbr(j, 2))], xg.at[piece(nbr(j, 3))], fwd_s.at[1, j], arr2.at[1, j], other)

    def x_on(j):
        return remote(xg.at[piece(nbr(j, 0)), 0:HALF], xg.at[piece(diag(j, 0)), 0:HALF], fwd_s.at[2, j], arr2.at[2, j], dev_y)

    def y_on(j):
        return remote(xg.at[piece(nbr(j, 2)), HALF:D], xg.at[piece(diag(j, 0)), HALF:D], fwd_s.at[3, j], arr2.at[3, j], dev_x)

    def d_other(j):
        return remote(xg.at[piece(diag(j, 0))], xg.at[piece(diag(j, 1))], fwd_s.at[4, j], arr2.at[4, j], other)

    def pass_on(j):
        x_on(j).wait_recv()
        y_on(j).wait_recv()
        d_other(j).start()

    gain = gain_v[...].reshape(1, D).astype(f32)
    SUB = 32
    per = CH // SUB

    def norm(i, _):
        rows = pl.ds(pl.multiple_of(i * SUB, SUB), SUB)
        p = i // per
        wide = vt[p // 2, pl.ds(pl.multiple_of(lax.rem(p, 2) * CH + lax.rem(i, per) * SUB, SUB), SUB), :].astype(f32)
        scale = lax.rsqrt(jnp.mean(wide * wide, -1, keepdims=True) + EPS)
        xg[rows, :] = (wide * scale * gain).astype(bf16)

    lax.fori_loop(0, per, norm, None)
    pl.semaphore_wait(barrier, 3)
    for j in range(NCH):
        own_x(j).start()
        own_y(j).start()
        own_other(j).start()
        if j + 1 < NCH:
            lxs[j + 1].wait()
            lax.fori_loop((j + 1) * per, (j + 2) * per, norm, None)
    wo_copy = remote(wo_ref, wo.at[WIDTH : 2 * WIDTH], wo_s.at[0], wo_s.at[1], other)
    wo_copy.start()
    for h in range(2):
        vt[h, HEAD : HEAD + SUMS, :] = jnp.ones((SUMS, SEQ), bf16)
    for c in (*lws, lnear, lfar):
        c.wait()

    def chunk_of(p):
        mine, theirs = 2 * chip + core, 2 * chip + 1 - core
        n = jnp.maximum(p - 2 * NCH, 0)
        nj, ni = n // 4, lax.rem(n, 4)
        nd = 2 * jnp.where(ni < 2, chip_x, chip_y) + jnp.where(lax.rem(ni, 2) == 0, core, 1 - core)
        m = jnp.maximum(p - 6 * NCH, 0)
        mj, mi = m // 2, lax.rem(m, 2)
        md = 2 * chip_d + jnp.where(mi == 0, core, 1 - core)
        at = jnp.where(p < NCH, mine * NCH + p, theirs * NCH + p - NCH)
        at = jnp.where(p >= 2 * NCH, nd * NCH + nj, at)
        return jnp.where(p >= 6 * NCH, md * NCH + mj, at)

    def project(b):
        @pl.when(b == 1)
        def _():
            own_other(0).wait_recv()

        @pl.when(b == 2)
        def _():
            own_other(1).wait_recv()
            own_other(2).wait_recv()

        for j in range(NCH):

            @pl.when(b == NCH + 2 * j)
            def _():
                own_x(j).wait_recv()
                x_other(j).start()
                x_on(j).start()
                own_y(j).wait_recv()
                y_other(j).start()
                y_on(j).start()
                x_other(j).wait_recv()

            @pl.when(b == NCH + 2 * j + 1)
            def _():
                y_other(j).wait_recv()

            @pl.when(b == 3 * NCH + j)
            def _():
                if j < NCH - 1:
                    pass_on(j)
                d_other(j).wait_recv()

        rows = xg[pl.ds(pl.multiple_of(b * 2 * CH, 2 * CH), 2 * CH), :]
        places, trig = [], []
        for i in range(2):
            at = chunk_of(2 * b + i)
            places.append(pl.ds(pl.multiple_of(at * CH, CH), CH))
            cf, sf = far_v[0, pl.ds(at, 1), :], far_v[1, pl.ds(at, 1), :]
            cn, sn = near_v[0], near_v[1]
            trig.append((cf * cn - sf * sn, sf * cn + cf * sn))
        for n, to in ((0, q), (1, k)):
            for h in range(2):
                t = dot(rows, w[n, :, h * HEAD : (h + 1) * HEAD]).astype(bf16).astype(f32)
                for i in range(2):
                    a, b_ = t[i * CH : (i + 1) * CH, : HEAD // 2], t[i * CH : (i + 1) * CH, HEAD // 2 :]
                    cos, sin = trig[i]
                    to[h, places[i], :] = jnp.concatenate([a * cos - b_ * sin, b_ * cos + a * sin], -1).astype(bf16)
        for h in range(2):
            t = dot(rows, w[2, :, h * HEAD : (h + 1) * HEAD]).astype(bf16)
            for i in range(2):
                vt[h, 0:HEAD, places[i]] = t[i * CH : (i + 1) * CH].T

    def place(i):
        return pl.ds(pl.multiple_of(i * WIDTH, WIDTH), WIDTH)

    def attention(i, to, strips=range(NS)):
        pieces = [(h, s) for h in range(2) for s in strips]
        q0 = pl.multiple_of(to * CHIP, CHIP)
        for n in range(len(pieces)):
            top_s[n : n + 1, :] = jnp.full((1, STRIP), NEG, f32)
            mix_s[n] = jnp.zeros(mix_s.shape[1:], f32)

        def block(k0, masked):
            def score(n):
                h, s = pieces[n]
                keys = (s + 1) * STRIP if masked else CHIP
                return dot(k[h, pl.ds(k0, keys), :], q[h, pl.ds(q0 + s * STRIP, STRIP), :], 1, 1)

            def soften(n, sc):
                s = pieces[n][1]
                if masked:
                    ok = (lax.broadcasted_iota(jnp.int32, sc.shape, 0) - s * STRIP) <= lax.broadcasted_iota(jnp.int32, sc.shape, 1)
                    sc = jnp.where(ok, sc, 2 * NEG)
                old = top_s[n : n + 1, :]
                top = jnp.maximum(old, sc.max(axis=0, keepdims=True))
                top_s[n : n + 1, :] = top
                return jnp.exp2((sc - top) * E2).astype(bf16), jnp.exp2((old - top) * E2)

            def mix(n, p, keep):
                h, s = pieces[n]
                keys = (s + 1) * STRIP if masked else CHIP
                mix_s[n] = mix_s[n] * keep + dot(vt[h, :, pl.ds(k0, keys)], p)

            count = len(pieces)
            scores = {n: score(n) for n in range(min(AHEAD, count))}
            held = None
            for n in range(count):
                soft = soften(n, scores.pop(n))
                if held is not None:
                    mix(n - 1, *held)
                held = soft
                if n + AHEAD < count:
                    scores[n + AHEAD] = score(n + AHEAD)
            mix(count - 1, *held)

        lax.fori_loop(0, to, lambda j, _: block(pl.multiple_of(j * CHIP, CHIP), False), None)
        block(q0, True)
        for n, (h, s) in enumerate(pieces):
            out = mix_s[n, 0:HEAD, :] * (1 / mix_s[n, HEAD : HEAD + 1, :])
            xg[s * STRIP : (s + 1) * STRIP, pl.ds(pl.multiple_of(i * WIDTH + h * HEAD, HEAD), HEAD)] = out.T.astype(bf16)

    def part(of, p):
        return pl.ds(pl.multiple_of(jnp.where(p == 0, of * CH, (1 - of) * STRIP), CH), CH if p else STRIP)

    def results(of, p=None):
        if p is None:
            return pl.ds(pl.multiple_of(of * ROWS, ROWS), ROWS)
        rows = part(of, p)
        return pl.ds(pl.multiple_of(of * ROWS + rows.start, CH), rows.size)

    def exchange(i):
        return remote(xg.at[results(1 - core), place(i)], pb.at[i], ex_s.at[0, i], ex_s.at[1, i], other)

    def exchange_part(p):
        slot = 4 if p else 2
        return remote(xg.at[results(1 - core, p), place(2)], pb.at[2, part(1 - core, p)], ex_s.at[0, slot], ex_s.at[1, slot], other)

    def term(i, t, p=None):
        mine = xg[results(core, p), place(i)]
        theirs = pb[i] if p is None else pb[i, part(core, p)]
        return dot(jnp.concatenate([mine, theirs], axis=1), wo[:, cols(t)])

    def cols(t):
        return pl.ds(pl.multiple_of(t * TILE, TILE), TILE)

    SX, SY, SD = (slice(n * ROWS, (n + 1) * ROWS) for n in range(2, 5))
    SUMS_IN = slice(5 * ROWS, 6 * ROWS)
    RD, DIR = (slice(n * ROWS, (n + 1) * ROWS) for n in range(6, 8))
    lxr = pltpu.make_async_copy(x_ref, o_ref, load.at[0])

    def send_xd(t):
        return remote(xg.at[SX, cols(t)], direct_h.at[:, cols(t)], rs_s.at[0, t], rs_r.at[0, t], dev_x)

    def send_yd(t):
        rows, at = pl.ds(pl.multiple_of(t // 2 * ROWS, ROWS), ROWS), cols(4 + lax.rem(t, 2))
        return remote(xg.at[rows, at], direct_h.at[:, cols(HT + t)], rs_s.at[1, HT + t], rs_r.at[1, HT + t], dev_y)

    def send_x(t):
        return remote(xg.at[SX, cols(HT + t)], xg.at[SUMS_IN, cols(HT + t)], rs_s.at[0, HT + t], rs_r.at[0, HT + t], dev_x)

    def send_y(t):
        return remote(xg.at[SY, cols(t)], xg.at[SUMS_IN, cols(t)], rs_s.at[1, t], rs_r.at[1, t], dev_y)

    def fetch_d(t):
        return pltpu.make_async_copy(diag_h.at[:, cols(t)], xg.at[RD, cols(t)], fetch.at[0, t])

    def fetch_direct(t):
        return pltpu.make_async_copy(direct_h.at[:, cols(t)], xg.at[DIR, cols(t)], fetch.at[1, t])

    def staged(p):
        rows = part(core, p)
        return pl.ds(pl.multiple_of(SD.start + rows.start, CH), rows.size)

    def send_d(t, p):
        return remote(xg.at[staged(p), cols(t)], diag_h.at[part(core, p), cols(t)], rs_s.at[2 + p, t], rs_r.at[2 + p, t], dev_x)

    def send_e(t, p):
        return remote(xg.at[staged(p), cols(t)], diag_h.at[part(core, p), cols(t)], rs_s.at[2 + p, t], rs_r.at[2 + p, t], dev_y)

    def diagonal(p):
        rows = staged(p)

        def one(t, _):
            xg[rows, cols(t)] = term(2, t, p).astype(bf16)
            send_d(t, p).start()
            xg[rows, cols(HT + t)] = term(2, HT + t, p).astype(bf16)
            send_e(HT + t, p).start()

        lax.fori_loop(0, HT, one, None)

    def item(n):
        x_first = chip_x < chip_y
        to = jnp.where(n == 2, chip, jnp.where((n == 0) == x_first, chip_x, chip_y))
        i = jnp.where(n == 2, 3, jnp.where((n == 0) == x_first, 0, 1))
        attention(i, to)
        ex = exchange(i)
        ex.start()

        @pl.when(n == 0)
        def _():
            for c in (x_other, y_other, x_on, y_on):
                c(0).wait_send()

        ex.wait_recv()

        def direct(t, _):
            tx, ty = t, HT + t

            @pl.when(i == 0)
            def _():
                xg[SX, cols(tx)] = term(0, tx).astype(bf16)
                send_xd(t).start()

            @pl.when(i == 1)
            def _():
                xg[pl.ds(pl.multiple_of(t // 2 * ROWS, ROWS), ROWS), cols(4 + lax.rem(t, 2))] = term(1, ty).astype(bf16)
                send_yd(t).start()

        lax.fori_loop(0, jnp.where(i == 3, 0, HT), direct, None)

    early = jnp.where(chip == 0, 2, jnp.where(chip == 3, 0, 1))
    first = 3 * NCH
    late = first + NCH + 2

    def step(n, _):
        @pl.when(n == first)
        def _():
            lwo.wait()
            wo_copy.wait()
            for j in range(NCH):
                for c in (own_other, own_x, own_y):
                    c(j).wait_send()

        m = n - early
        is_item = ((n >= first) & (n < first + early)) | (m >= late)
        on = (n < first) | (m >= first)

        @pl.when((n < first) | ((m >= first) & (m < first + 2)) | (m == first + 3))
        def _():
            project(jnp.where(n < first, n, jnp.where(m == first + 3, first + 2, m)))

        @pl.when(on & (m == first + 2) & (n >= first))
        def _():
            attention(2, chip_d, range(1))

            @pl.when(core == 1)
            def _():
                exchange_part(0).start()

            pass_on(NCH - 1)
            for j in range(1, NCH):
                for c in (x_other, y_other, x_on, y_on):
                    c(j).wait_send()
            lxr.start()

            @pl.when(core == 0)
            def _():
                exchange_part(0).wait_recv()
                diagonal(0)

        @pl.when(on & (m == first + 4) & (n >= first))
        def _():
            for to in (dev_x, dev_y):
                pl.semaphore_signal(free, inc=1, device_id={"tp": to}, device_id_type=pl.DeviceIdType.MESH)
            for j in range(NCH):
                d_other(j).wait_send()
            attention(2, chip_d, range(1, 2))
            exchange_part(1).start()
            at_once = (core == 0) & (chip != 3)

            @pl.when(at_once)
            def _():
                exchange_part(1).wait_recv()
                diagonal(1)

            attention(2, chip_d, range(2, 3))

            @pl.when(core == 0)
            def _():
                exchange_part(0).start()

            @pl.when(jnp.logical_not(at_once))
            def _():
                exchange_part(1).wait_recv()
                diagonal(1)

            @pl.when(core == 1)
            def _():
                exchange_part(0).wait_recv()
                diagonal(0)

        @pl.when(is_item)
        def _():
            item(jnp.where(n < first + early, n - first, m - late + early))

    lax.fori_loop(0, late + 3, step, None)

    def combine(t, _):
        tx, ty = HT + t, t
        send_e(tx, 0).wait_recv()
        send_e(tx, 1).wait_recv()
        fetch_d(tx).start()
        fetch_d(tx).wait()
        xg[SX, cols(tx)] = (term(0, tx) + xg[RD, cols(tx)].astype(f32)).astype(bf16)
        send_x(t).start()
        send_d(ty, 0).wait_recv()
        send_d(ty, 1).wait_recv()
        fetch_d(ty).start()
        fetch_d(ty).wait()
        xg[SY, cols(ty)] = (term(1, ty) + xg[RD, cols(ty)].astype(f32)).astype(bf16)
        send_y(t).start()

    pl.semaphore_wait(free, 2)
    lax.fori_loop(0, HT, combine, None)

    for t in range(HT):
        send_xd(t).wait_recv()
        fetch_direct(t).start()
        send_yd(t).wait_recv()
        fetch_direct(HT + t).start()
    lxr.wait()
    for t in range(2 * HT):
        fetch_direct(t).wait()

    def finish(t, _):
        def known(t):
            return o_ref[:, cols(t)].astype(f32) + (term(3, t) + xg[DIR, cols(t)].astype(f32))

        def add(t, total):
            o_ref[:, cols(t)] = (total + xg[SUMS_IN, cols(t)].astype(f32)).astype(bf16)

        left, right = known(t), known(HT + t)
        send_y(t).wait_recv()
        add(t, left)
        send_x(t).wait_recv()
        add(HT + t, right)

    lax.fori_loop(0, HT, finish, None)
    for t in range(HT):
        for c in (send_xd, send_yd, send_x, send_y):
            c(t).wait_send()
        for p in range(2):
            send_d(t, p).wait_send()
            send_e(HT + t, p).wait_send()
    for i in (0, 1, 3):
        exchange(i).wait_send()
    for p in range(2):
        exchange_part(p).wait_send()


def in_hbm(a):
    return pltpu.with_memory_space_constraint(jnp.asarray(a), pltpu.HBM)


def solution(mesh):
    def step(x, gain, wq, wk, wv, wo):
        rate = THETA ** (-np.arange(HEAD // 2) / (HEAD // 2))
        near = np.arange(CH)[:, None] * rate
        far = (np.arange(SEQ // CH) * CH)[:, None] * rate
        near, far = (np.stack([np.cos(a), np.sin(a)]).astype(np.float32) for a in (near, far))
        hbm = pl.BlockSpec(memory_space=pltpu.HBM)
        dma, V = pltpu.SemaphoreType.DMA, pltpu.VMEM
        return pl.pallas_call(
            kernel,
            out_shape=[jax.ShapeDtypeStruct((ROWS, D), bf16)] * 3,
            in_specs=[hbm] * 8,
            out_specs=[pl.BlockSpec(memory_space=pltpu.VMEM), hbm, hbm],
            scratch_shapes=[
                V((SEQ, D), bf16),
                V((3, D, WIDTH), bf16),
                V((2 * WIDTH, D), bf16),
                V((2, SEQ, HEAD), bf16),
                V((2, SEQ, HEAD), bf16),
                V((2, HEAD + SUMS, SEQ), bf16),
                V((4, ROWS, WIDTH), bf16),
                V((8, STRIP), f32),
                V((2 * NS, HEAD + SUMS, STRIP), f32),
                V((D,), bf16), V(near.shape, f32), V(far.shape, f32),
                dma((8 + NCH,)), dma((3, NCH)), dma((3, NCH)), dma((5, NCH)), dma((5, NCH)), dma((2,)), dma((2, 5)),
                dma((4, 2 * HT)), dma((4, 2 * HT)), dma((2, 2 * HT)), pltpu.SemaphoreType.REGULAR,
            ],
            compiler_params=pltpu.CompilerParams(collective_id=0, has_side_effects=True, vmem_limit_bytes=53_900_000),
        )(x, in_hbm(gain), wq, wk, wv, wo, in_hbm(near), in_hbm(far))[0]

    tokens, columns = P(("dp", "tp"), None), P(None, "tp")
    return jax.shard_map(
        step,
        mesh=mesh,
        in_specs=(tokens, P(None), columns, columns, columns, P("tp", None)),
        out_specs=tokens,
        check_vma=False,
    )
```

```python
import functools

import jax
import jax.numpy as jnp
import numpy as np
from jax import lax
from jax.experimental import pallas as pl
from jax.experimental.pallas import tpu as pltpu
from jax.sharding import PartitionSpec as P

HEAD = 256
THETA = 10000
LOG2E = 1.4426950408889634
NEG = -1e30
EPS = 1e-6
CH = 128
NCH = 3
ROWS = CH * NCH
D = 3072
HALF = D // 2
TILE = 512
HT = HALF // TILE
SEQ = 8 * ROWS
CHIP = 2 * ROWS
STRIP = 256
NS = CHIP // STRIP
AHEAD = 3
SUMS = 8
WIDTH = 2 * HEAD
SCALE = HEAD**-0.5
E2 = SCALE * LOG2E

f32, bf16 = jnp.float32, jnp.bfloat16


def dot(a, b, ca=1, cb=0):
    return lax.dot_general(a, b, (((ca,), (cb,)), ((), ())), preferred_element_type=f32)


def kernel(x_ref, gain_ref, wq_ref, wk_ref, wv_ref, wo_ref, near_ref, far_ref, o_ref, diag_h, direct_h,
           xg, w, wo, q, k, vt, pb, top_s, mix_s, gain_v, near_v, far_v,
           load, own_s, arr, fwd_s, arr2, wo_s, ex_s, rs_s, rs_r, fetch, free):
    me = lax.axis_index("tp")
    chip = me // 2
    core = me - 2 * chip
    chip_x = lax.rem(chip + 2, 4)
    chip_y = chip + 1 - 2 * lax.rem(chip, 2)
    chip_d = 3 - chip
    other, dev_x, dev_y = 2 * chip + 1 - core, 2 * chip_x + core, 2 * chip_y + core

    def remote(src, dst, s, r, to):
        return pltpu.make_async_remote_copy(src_ref=src, dst_ref=dst, send_sem=s, recv_sem=r, device_id={"tp": to},
                                            device_id_type=pl.DeviceIdType.MESH)

    def piece(p):
        return pl.ds(pl.multiple_of(p * CH, CH), CH)

    lgain = pltpu.make_async_copy(gain_ref, gain_v, load.at[5])
    lgain.start()
    lxs = [pltpu.make_async_copy(x_ref.at[piece(j)], vt.at[j // 2, j % 2 * CH : (j % 2 + 1) * CH], load.at[8 + j]) for j in range(NCH)]
    for c in lxs:
        c.start()
    lnear, lfar = pltpu.make_async_copy(near_ref, near_v, load.at[6]), pltpu.make_async_copy(far_ref, far_v, load.at[7])
    lnear.start()
    lfar.start()
    lws = [pltpu.make_async_copy(r, w.at[i], load.at[1 + i]) for i, r in enumerate((wq_ref, wk_ref, wv_ref))]
    for c in lws:
        c.start()
    lwo = pltpu.make_async_copy(wo_ref, wo.at[0:WIDTH], load.at[4])
    lwo.start()

    barrier = pltpu.get_barrier_semaphore()
    for to in (other, dev_x, dev_y):
        pl.semaphore_signal(barrier, inc=1, device_id={"tp": to}, device_id_type=pl.DeviceIdType.MESH)
    lgain.wait()
    lxs[0].wait()

    def nbr(j, i):
        return 2 * NCH + 4 * j + i

    def diag(j, i):
        return 6 * NCH + 2 * j + i

    def own_other(j):
        return remote(xg.at[piece(j)], xg.at[piece(NCH + j)], own_s.at[0, j], arr.at[0, j], other)

    def own_x(j):
        return remote(xg.at[piece(j)], xg.at[piece(nbr(j, 0))], own_s.at[1, j], arr.at[1, j], dev_x)

    def own_y(j):
        return remote(xg.at[piece(j)], xg.at[piece(nbr(j, 2))], own_s.at[2, j], arr.at[2, j], dev_y)

    def x_other(j):
        return remote(xg.at[piece(nbr(j, 0))], xg.at[piece(nbr(j, 1))], fwd_s.at[0, j], arr2.at[0, j], other)

    def y_other(j):
        return remote(xg.at[piece(nbr(j, 2))], xg.at[piece(nbr(j, 3))], fwd_s.at[1, j], arr2.at[1, j], other)

    def x_on(j):
        return remote(xg.at[piece(nbr(j, 0)), 0:HALF], xg.at[piece(diag(j, 0)), 0:HALF], fwd_s.at[2, j], arr2.at[2, j], dev_y)

    def y_on(j):
        return remote(xg.at[piece(nbr(j, 2)), HALF:D], xg.at[piece(diag(j, 0)), HALF:D], fwd_s.at[3, j], arr2.at[3, j], dev_x)

    def d_other(j):
        return remote(xg.at[piece(diag(j, 0))], xg.at[piece(diag(j, 1))], fwd_s.at[4, j], arr2.at[4, j], other)

    def pass_on(j):
        x_on(j).wait_recv()
        y_on(j).wait_recv()
        d_other(j).start()

    gain = gain_v[...].reshape(1, D).astype(f32)
    SUB = 32
    per = CH // SUB

    def norm(i, _):
        rows = pl.ds(pl.multiple_of(i * SUB, SUB), SUB)
        p = i // per
        wide = vt[p // 2, pl.ds(pl.multiple_of(lax.rem(p, 2) * CH + lax.rem(i, per) * SUB, SUB), SUB), :].astype(f32)
        scale = lax.rsqrt(jnp.mean(wide * wide, -1, keepdims=True) + EPS)
        xg[rows, :] = (wide * scale * gain).astype(bf16)

    lax.fori_loop(0, per, norm, None)
    pl.semaphore_wait(barrier, 3)
    for j in range(NCH):
        own_x(j).start()
        own_y(j).start()
        own_other(j).start()
        if j + 1 < NCH:
            lxs[j + 1].wait()
            lax.fori_loop((j + 1) * per, (j + 2) * per, norm, None)
    wo_copy = remote(wo_ref, wo.at[WIDTH : 2 * WIDTH], wo_s.at[0], wo_s.at[1], other)
    wo_copy.start()
    for h in range(2):
        vt[h, HEAD : HEAD + SUMS, :] = jnp.ones((SUMS, SEQ), bf16)
    for c in (*lws, lnear, lfar):
        c.wait()

    def chunk_of(p):
        mine, theirs = 2 * chip + core, 2 * chip + 1 - core
        n = jnp.maximum(p - 2 * NCH, 0)
        nj, ni = n // 4, lax.rem(n, 4)
        nd = 2 * jnp.where(ni < 2, chip_x, chip_y) + jnp.where(lax.rem(ni, 2) == 0, core, 1 - core)
        m = jnp.maximum(p - 6 * NCH, 0)
        mj, mi = m // 2, lax.rem(m, 2)
        md = 2 * chip_d + jnp.where(mi == 0, core, 1 - core)
        at = jnp.where(p < NCH, mine * NCH + p, theirs * NCH + p - NCH)
        at = jnp.where(p >= 2 * NCH, nd * NCH + nj, at)
        return jnp.where(p >= 6 * NCH, md * NCH + mj, at)

    def project(b):
        @pl.when(b == 1)
        def _():
            own_other(0).wait_recv()

        @pl.when(b == 2)
        def _():
            own_other(1).wait_recv()
            own_other(2).wait_recv()

        for j in range(NCH):

            @pl.when(b == NCH + 2 * j)
            def _():
                own_x(j).wait_recv()
                x_other(j).start()
                x_on(j).start()
                own_y(j).wait_recv()
                y_other(j).start()
                y_on(j).start()
                x_other(j).wait_recv()

            @pl.when(b == NCH + 2 * j + 1)
            def _():
                y_other(j).wait_recv()

        @pl.when(b == 3 * NCH)
        def _():
            pass_on(0)
            d_other(0).wait_recv()

        project_rows(2 * b, 2)

    def project_rows(p0, count):
        rows = xg[pl.ds(pl.multiple_of(p0 * CH, CH), count * CH), :]
        places, trig = [], []
        for i in range(count):
            at = chunk_of(p0 + i)
            places.append(pl.ds(pl.multiple_of(at * CH, CH), CH))
            cf, sf = far_v[0, pl.ds(at, 1), :], far_v[1, pl.ds(at, 1), :]
            cn, sn = near_v[0], near_v[1]
            trig.append((cf * cn - sf * sn, sf * cn + cf * sn))
        for n, to in ((0, q), (1, k)):
            for h in range(2):
                t = dot(rows, w[n, :, h * HEAD : (h + 1) * HEAD]).astype(bf16).astype(f32)
                for i in range(count):
                    a, b_ = t[i * CH : (i + 1) * CH, : HEAD // 2], t[i * CH : (i + 1) * CH, HEAD // 2 :]
                    cos, sin = trig[i]
                    to[h, places[i], :] = jnp.concatenate([a * cos - b_ * sin, b_ * cos + a * sin], -1).astype(bf16)
        for h in range(2):
            t = dot(rows, w[2, :, h * HEAD : (h + 1) * HEAD]).astype(bf16)
            for i in range(count):
                vt[h, 0:HEAD, places[i]] = t[i * CH : (i + 1) * CH].T

    def place(i):
        return pl.ds(pl.multiple_of(i * WIDTH, WIDTH), WIDTH)

    def attention(i, to, strips=range(NS)):
        pieces = [(h, s) for h in range(2) for s in strips]
        q0 = pl.multiple_of(to * CHIP, CHIP)
        for n in range(len(pieces)):
            top_s[n : n + 1, :] = jnp.full((1, STRIP), NEG, f32)
            mix_s[n] = jnp.zeros(mix_s.shape[1:], f32)

        def block(k0, masked):
            def score(n):
                h, s = pieces[n]
                keys = (s + 1) * STRIP if masked else CHIP
                return dot(k[h, pl.ds(k0, keys), :], q[h, pl.ds(q0 + s * STRIP, STRIP), :], 1, 1)

            def soften(n, sc):
                s = pieces[n][1]
                if masked:
                    ok = (lax.broadcasted_iota(jnp.int32, sc.shape, 0) - s * STRIP) <= lax.broadcasted_iota(jnp.int32, sc.shape, 1)
                    sc = jnp.where(ok, sc, 2 * NEG)
                old = top_s[n : n + 1, :]
                top = jnp.maximum(old, sc.max(axis=0, keepdims=True))
                top_s[n : n + 1, :] = top
                return jnp.exp2((sc - top) * E2).astype(bf16), jnp.exp2((old - top) * E2)

            def mix(n, p, keep):
                h, s = pieces[n]
                keys = (s + 1) * STRIP if masked else CHIP
                mix_s[n] = mix_s[n] * keep + dot(vt[h, :, pl.ds(k0, keys)], p)

            count = len(pieces)
            scores = {n: score(n) for n in range(min(AHEAD, count))}
            held = None
            for n in range(count):
                soft = soften(n, scores.pop(n))
                if held is not None:
                    mix(n - 1, *held)
                held = soft
                if n + AHEAD < count:
                    scores[n + AHEAD] = score(n + AHEAD)
            mix(count - 1, *held)

        lax.fori_loop(0, to, lambda j, _: block(pl.multiple_of(j * CHIP, CHIP), False), None)
        block(q0, True)
        for n, (h, s) in enumerate(pieces):
            out = mix_s[n, 0:HEAD, :] * (1 / mix_s[n, HEAD : HEAD + 1, :])
            xg[s * STRIP : (s + 1) * STRIP, pl.ds(pl.multiple_of(i * WIDTH + h * HEAD, HEAD), HEAD)] = out.T.astype(bf16)

    def part(of, p):
        return pl.ds(pl.multiple_of(jnp.where(p == 0, of * CH, (1 - of) * STRIP), CH), CH if p else STRIP)

    def results(of, p=None):
        if p is None:
            return pl.ds(pl.multiple_of(of * ROWS, ROWS), ROWS)
        rows = part(of, p)
        return pl.ds(pl.multiple_of(of * ROWS + rows.start, CH), rows.size)

    def exchange(i):
        return remote(xg.at[results(1 - core), place(i)], pb.at[i], ex_s.at[0, i], ex_s.at[1, i], other)

    def exchange_part(p):
        slot = 4 if p else 2
        return remote(xg.at[results(1 - core, p), place(2)], pb.at[2, part(1 - core, p)], ex_s.at[0, slot], ex_s.at[1, slot], other)

    def term(i, t, p=None):
        mine = xg[results(core, p), place(i)]
        theirs = pb[i] if p is None else pb[i, part(core, p)]
        return dot(jnp.concatenate([mine, theirs], axis=1), wo[:, cols(t)])

    def cols(t):
        return pl.ds(pl.multiple_of(t * TILE, TILE), TILE)

    SX, SY, SD = (slice(n * ROWS, (n + 1) * ROWS) for n in range(2, 5))
    SUMS_IN = slice(5 * ROWS, 6 * ROWS)
    RD, DIR = (slice(n * ROWS, (n + 1) * ROWS) for n in range(6, 8))
    lxr = pltpu.make_async_copy(x_ref, o_ref, load.at[0])

    def send_xd(t):
        return remote(xg.at[SX, cols(t)], direct_h.at[:, cols(t)], rs_s.at[0, t], rs_r.at[0, t], dev_x)

    def send_yd(t):
        rows, at = pl.ds(pl.multiple_of(t // 2 * ROWS, ROWS), ROWS), cols(4 + lax.rem(t, 2))
        return remote(xg.at[rows, at], direct_h.at[:, cols(HT + t)], rs_s.at[1, HT + t], rs_r.at[1, HT + t], dev_y)

    def send_x(t):
        return remote(xg.at[SX, cols(HT + t)], xg.at[SUMS_IN, cols(HT + t)], rs_s.at[0, HT + t], rs_r.at[0, HT + t], dev_x)

    def send_y(t):
        return remote(xg.at[SY, cols(t)], xg.at[SUMS_IN, cols(t)], rs_s.at[1, t], rs_r.at[1, t], dev_y)

    def fetch_d(t):
        return pltpu.make_async_copy(diag_h.at[:, cols(t)], xg.at[RD, cols(t)], fetch.at[0, t])

    def fetch_direct(t):
        return pltpu.make_async_copy(direct_h.at[:, cols(t)], xg.at[DIR, cols(t)], fetch.at[1, t])

    def staged(p):
        rows = part(core, p)
        return pl.ds(pl.multiple_of(SD.start + rows.start, CH), rows.size)

    def send_d(t, p):
        return remote(xg.at[staged(p), cols(t)], diag_h.at[part(core, p), cols(t)], rs_s.at[2 + p, t], rs_r.at[2 + p, t], dev_x)

    def send_e(t, p):
        return remote(xg.at[staged(p), cols(t)], diag_h.at[part(core, p), cols(t)], rs_s.at[2 + p, t], rs_r.at[2 + p, t], dev_y)

    def diagonal(p):
        lax.fori_loop(0, HT, functools.partial(diagonal_pieces, p), None)

    def diagonal_pieces(p, t, _):
        rows = staged(p)
        xg[rows, cols(t)] = term(2, t, p).astype(bf16)
        send_d(t, p).start()
        xg[rows, cols(HT + t)] = term(2, HT + t, p).astype(bf16)
        send_e(HT + t, p).start()

    def item(n):
        x_first = chip_x < chip_y
        to = jnp.where(n == 2, chip, jnp.where((n == 0) == x_first, chip_x, chip_y))
        i = jnp.where(n == 2, 3, jnp.where((n == 0) == x_first, 0, 1))
        attention(i, to)
        ex = exchange(i)
        ex.start()

        @pl.when(n == 0)
        def _():
            for c in (x_other, y_other, x_on, y_on):
                c(0).wait_send()

        ex.wait_recv()

        def direct(t, _):
            tx, ty = t, HT + t

            @pl.when(i == 0)
            def _():
                xg[SX, cols(tx)] = term(0, tx).astype(bf16)
                send_xd(t).start()

            @pl.when(i == 1)
            def _():
                xg[pl.ds(pl.multiple_of(t // 2 * ROWS, ROWS), ROWS), cols(4 + lax.rem(t, 2))] = term(1, ty).astype(bf16)
                send_yd(t).start()

        lax.fori_loop(0, jnp.where(i == 3, 0, HT), direct, None)

    early = jnp.where(chip == 0, 2, jnp.where(chip == 3, 0, 1))
    first = 3 * NCH
    late = first + 3

    def step(n, _):
        @pl.when(n == first)
        def _():
            lwo.wait()
            wo_copy.wait()
            for j in range(NCH):
                for c in (own_other, own_x, own_y):
                    c(j).wait_send()

        m = n - early
        is_item = ((n >= first) & (n < first + early)) | (m >= late)
        on = (n < first) | (m >= first)

        @pl.when((n < first) | (on & (m == first)))
        def _():
            project(jnp.where(n < first, n, first))

        def diagonal_rows(j, of):
            @pl.when(core != of)
            def _():
                d_other(j).wait_recv()

            project_rows(diag(j, jnp.where(core == of, 0, 1)), 1)

        @pl.when(on & (m == first + 1))
        def _():
            pass_on(1)
            diagonal_rows(1, 0)
            attention(2, chip_d, range(1))

            @pl.when(core == 1)
            def _():
                exchange_part(0).start()

            diagonal_rows(1, 1)
            for c in (x_other, y_other, x_on, y_on):
                c(1).wait_send()

            @pl.when(core == 0)
            def _():
                exchange_part(0).wait_recv()
                diagonal_pieces(0, 0, None)

            pass_on(2)
            for c in (x_other, y_other, x_on, y_on):
                c(2).wait_send()
            lxr.start()

            @pl.when(core == 0)
            def _():
                lax.fori_loop(1, HT, functools.partial(diagonal_pieces, 0), None)

        @pl.when(on & (m == first + 2))
        def _():
            diagonal_rows(2, 0)
            attention(2, chip_d, range(1, 2))
            exchange_part(1).start()
            diagonal_rows(2, 1)
            at_once = (core == 0) & (chip != 3)

            @pl.when(at_once)
            def _():
                exchange_part(1).wait_recv()
                diagonal(1)

            for to in (dev_x, dev_y):
                pl.semaphore_signal(free, inc=1, device_id={"tp": to}, device_id_type=pl.DeviceIdType.MESH)
            for j in range(NCH):
                d_other(j).wait_send()
            attention(2, chip_d, range(2, 3))

            @pl.when(core == 0)
            def _():
                exchange_part(0).start()

            @pl.when(jnp.logical_not(at_once))
            def _():
                exchange_part(1).wait_recv()
                diagonal(1)

            @pl.when(core == 1)
            def _():
                exchange_part(0).wait_recv()
                diagonal(0)

        @pl.when(is_item)
        def _():
            item(jnp.where(n < first + early, n - first, m - late + early))

    lax.fori_loop(0, late + 3, step, None)

    def combine(t, _):
        tx, ty = HT + t, t
        send_e(tx, 0).wait_recv()
        send_e(tx, 1).wait_recv()
        fetch_d(tx).start()
        fetch_d(tx).wait()
        xg[SX, cols(tx)] = (term(0, tx) + xg[RD, cols(tx)].astype(f32)).astype(bf16)
        send_x(t).start()
        send_d(ty, 0).wait_recv()
        send_d(ty, 1).wait_recv()
        fetch_d(ty).start()
        fetch_d(ty).wait()
        xg[SY, cols(ty)] = (term(1, ty) + xg[RD, cols(ty)].astype(f32)).astype(bf16)
        send_y(t).start()

    pl.semaphore_wait(free, 2)
    lax.fori_loop(0, HT, combine, None)

    for t in range(HT):
        send_xd(t).wait_recv()
        fetch_direct(t).start()
        send_yd(t).wait_recv()
        fetch_direct(HT + t).start()
    lxr.wait()
    for t in range(2 * HT):
        fetch_direct(t).wait()

    def finish(t, _):
        def known(t):
            return o_ref[:, cols(t)].astype(f32) + (term(3, t) + xg[DIR, cols(t)].astype(f32))

        def add(t, total):
            o_ref[:, cols(t)] = (total + xg[SUMS_IN, cols(t)].astype(f32)).astype(bf16)

        left, right = known(t), known(HT + t)
        send_y(t).wait_recv()
        add(t, left)
        send_x(t).wait_recv()
        add(HT + t, right)

    lax.fori_loop(0, HT, finish, None)
    for t in range(HT):
        for c in (send_xd, send_yd, send_x, send_y):
            c(t).wait_send()
        for p in range(2):
            send_d(t, p).wait_send()
            send_e(HT + t, p).wait_send()
    for i in (0, 1, 3):
        exchange(i).wait_send()
    for p in range(2):
        exchange_part(p).wait_send()


def in_hbm(a):
    return pltpu.with_memory_space_constraint(jnp.asarray(a), pltpu.HBM)


def solution(mesh):
    def step(x, gain, wq, wk, wv, wo):
        rate = THETA ** (-np.arange(HEAD // 2) / (HEAD // 2))
        near = np.arange(CH)[:, None] * rate
        far = (np.arange(SEQ // CH) * CH)[:, None] * rate
        near, far = (np.stack([np.cos(a), np.sin(a)]).astype(np.float32) for a in (near, far))
        hbm = pl.BlockSpec(memory_space=pltpu.HBM)
        dma, V = pltpu.SemaphoreType.DMA, pltpu.VMEM
        return pl.pallas_call(
            kernel,
            out_shape=[jax.ShapeDtypeStruct((ROWS, D), bf16)] * 3,
            in_specs=[hbm] * 8,
            out_specs=[pl.BlockSpec(memory_space=pltpu.VMEM), hbm, hbm],
            scratch_shapes=[
                V((SEQ, D), bf16),
                V((3, D, WIDTH), bf16),
                V((2 * WIDTH, D), bf16),
                V((2, SEQ, HEAD), bf16),
                V((2, SEQ, HEAD), bf16),
                V((2, HEAD + SUMS, SEQ), bf16),
                V((4, ROWS, WIDTH), bf16),
                V((8, STRIP), f32),
                V((2 * NS, HEAD + SUMS, STRIP), f32),
                V((D,), bf16), V(near.shape, f32), V(far.shape, f32),
                dma((8 + NCH,)), dma((3, NCH)), dma((3, NCH)), dma((5, NCH)), dma((5, NCH)), dma((2,)), dma((2, 5)),
                dma((4, 2 * HT)), dma((4, 2 * HT)), dma((2, 2 * HT)), pltpu.SemaphoreType.REGULAR,
            ],
            compiler_params=pltpu.CompilerParams(collective_id=0, has_side_effects=True, vmem_limit_bytes=53_900_000),
        )(x, in_hbm(gain), wq, wk, wv, wo, in_hbm(near), in_hbm(far))[0]

    tokens, columns = P(("dp", "tp"), None), P(None, "tp")
    return jax.shard_map(
        step,
        mesh=mesh,
        in_specs=(tokens, P(None), columns, columns, columns, P("tp", None)),
        out_specs=tokens,
        check_vma=False,
    )
```

```python
import functools

import jax
import jax.numpy as jnp
import numpy as np
from jax import lax
from jax.experimental import pallas as pl
from jax.experimental.pallas import tpu as pltpu
from jax.sharding import PartitionSpec as P

HEAD = 256
THETA = 10000
LOG2E = 1.4426950408889634
NEG = -1e30
EPS = 1e-6
CH = 128
NCH = 3
SUB = 32
ROWS = CH * NCH
D = 3072
HALF = D // 2
TILE = 512
HT = HALF // TILE
SEQ = 8 * ROWS
CHIP = 2 * ROWS
STRIP = 256
NS = CHIP // STRIP
AHEAD = 3
SUMS = 8
WIDTH = 2 * HEAD
SCALE = HEAD**-0.5
E2 = SCALE * LOG2E

f32, bf16 = jnp.float32, jnp.bfloat16


def dot(a, b, ca=1, cb=0):
    return lax.dot_general(a, b, (((ca,), (cb,)), ((), ())), preferred_element_type=f32)


def kernel(x_ref, gain_ref, wq_ref, wk_ref, wv_ref, wo_ref, near_ref, far_ref, o_ref, diag_h, direct_h,
           xg, w, wo, q, k, vt, pb, top_s, mix_s, gain_v, near_v, far_v,
           load, own_s, arr, fwd_s, arr2, wo_s, ex_s, rs_s, rs_r, fetch, free):
    me = lax.axis_index("tp")
    chip = me // 2
    core = me - 2 * chip
    chip_x = lax.rem(chip + 2, 4)
    chip_y = chip + 1 - 2 * lax.rem(chip, 2)
    chip_d = 3 - chip
    other, dev_x, dev_y = 2 * chip + 1 - core, 2 * chip_x + core, 2 * chip_y + core

    def remote(src, dst, s, r, to):
        return pltpu.make_async_remote_copy(src_ref=src, dst_ref=dst, send_sem=s, recv_sem=r, device_id={"tp": to},
                                            device_id_type=pl.DeviceIdType.MESH)

    def piece(p):
        return pl.ds(pl.multiple_of(p * CH, CH), CH)

    lgain = pltpu.make_async_copy(gain_ref, gain_v, load.at[3])
    lgain.start()
    lxs = [pltpu.make_async_copy(x_ref.at[piece(j)], vt.at[j // 2, j % 2 * CH : (j % 2 + 1) * CH], load.at[6 + j]) for j in range(NCH)]
    for c in lxs:
        c.start()
    lnear, lfar = pltpu.make_async_copy(near_ref, near_v, load.at[4]), pltpu.make_async_copy(far_ref, far_v, load.at[5])
    lnear.start()
    lfar.start()
    lws = [pltpu.make_async_copy(r, w.at[i], load.at[1]) for i, r in enumerate((wq_ref, wk_ref, wv_ref))]
    for c in lws:
        c.start()
    lwo = pltpu.make_async_copy(wo_ref, wo.at[0:WIDTH], load.at[2])
    lwo.start()

    barrier = pltpu.get_barrier_semaphore()
    for to in (other, dev_x, dev_y):
        pl.semaphore_signal(barrier, inc=1, device_id={"tp": to}, device_id_type=pl.DeviceIdType.MESH)
    lgain.wait()
    lxs[0].wait()

    def nbr(j, i):
        return 2 * NCH + 4 * j + i

    def diag(j, i):
        return 6 * NCH + 2 * j + i

    def sent(rows, s):
        remote(xg.at[0:rows], xg.at[0:rows], s, wo_s.at[1], other).wait_send()

    def own_other(j):
        return remote(xg.at[piece(j)], xg.at[piece(NCH + j)], own_s.at[0], arr.at[0, j], other)

    def own_rest(j, at, r, to):
        skip = 0 if j else SUB
        return remote(xg.at[pl.ds(j * CH + skip, CH - skip)], xg.at[pl.ds(nbr(j, at) * CH + skip, CH - skip)], own_s.at[0], r, to)

    def own_first(at, r, to):
        return remote(xg.at[pl.ds(0, SUB)], xg.at[pl.ds(nbr(0, at) * CH, SUB)], own_s.at[0], r, to)

    def own_x(j):
        return own_rest(j, 0, arr.at[1, j], dev_x)

    def own_y(j):
        return own_rest(j, 2, arr.at[2, j], dev_y)

    first_x, first_y = own_first(0, arr.at[1, NCH], dev_x), own_first(2, arr.at[2, NCH], dev_y)

    def x_other(j):
        return remote(xg.at[piece(nbr(j, 0))], xg.at[piece(nbr(j, 1))], fwd_s.at[j], arr2.at[0, j], other)

    def y_other(j):
        return remote(xg.at[piece(nbr(j, 2))], xg.at[piece(nbr(j, 3))], fwd_s.at[j], arr2.at[1, j], other)

    def x_on(j):
        return remote(xg.at[piece(nbr(j, 0)), 0:HALF], xg.at[piece(diag(j, 0)), 0:HALF], fwd_s.at[j], arr2.at[2, j], dev_y)

    def y_on(j):
        return remote(xg.at[piece(nbr(j, 2)), HALF:D], xg.at[piece(diag(j, 0)), HALF:D], fwd_s.at[j], arr2.at[3, j], dev_x)

    def d_other(j):
        return remote(xg.at[piece(diag(j, 0))], xg.at[piece(diag(j, 1))], fwd_s.at[NCH], arr2.at[4, j], other)

    def pass_on(j):
        x_on(j).wait_recv()
        y_on(j).wait_recv()
        d_other(j).start()

    gain = gain_v[...].reshape(1, D).astype(f32)
    per = CH // SUB

    def norm(i, _):
        rows = pl.ds(pl.multiple_of(i * SUB, SUB), SUB)
        p = i // per
        wide = vt[p // 2, pl.ds(pl.multiple_of(lax.rem(p, 2) * CH + lax.rem(i, per) * SUB, SUB), SUB), :].astype(f32)
        scale = lax.rsqrt(jnp.mean(wide * wide, -1, keepdims=True) + EPS)
        xg[rows, :] = (wide * scale * gain).astype(bf16)

    norm(0, None)
    pl.semaphore_wait(barrier, 3)
    first_x.start()
    first_y.start()
    lax.fori_loop(1, per, norm, None)
    for j in range(NCH):
        own_x(j).start()
        own_y(j).start()
        own_other(j).start()
        if j + 1 < NCH:
            lxs[j + 1].wait()
            lax.fori_loop((j + 1) * per, (j + 2) * per, norm, None)
    wo_copy = remote(wo_ref, wo.at[WIDTH : 2 * WIDTH], wo_s.at[0], wo_s.at[1], other)
    wo_copy.start()
    for h in range(2):
        vt[h, HEAD : HEAD + SUMS, :] = jnp.ones((SUMS, SEQ), bf16)
    pltpu.make_async_copy(w, w, load.at[1]).wait()
    lnear.wait()
    lfar.wait()

    def chunk_of(p):
        mine, theirs = 2 * chip + core, 2 * chip + 1 - core
        n = jnp.maximum(p - 2 * NCH, 0)
        nj, ni = n // 4, lax.rem(n, 4)
        nd = 2 * jnp.where(ni < 2, chip_x, chip_y) + jnp.where(lax.rem(ni, 2) == 0, core, 1 - core)
        m = jnp.maximum(p - 6 * NCH, 0)
        mj, mi = m // 2, lax.rem(m, 2)
        md = 2 * chip_d + jnp.where(mi == 0, core, 1 - core)
        at = jnp.where(p < NCH, mine * NCH + p, theirs * NCH + p - NCH)
        at = jnp.where(p >= 2 * NCH, nd * NCH + nj, at)
        return jnp.where(p >= 6 * NCH, md * NCH + mj, at)

    def project(b):
        @pl.when(b == 1)
        def _():
            own_other(0).wait_recv()

        @pl.when(b == 2)
        def _():
            own_other(1).wait_recv()
            own_other(2).wait_recv()

        for j in range(NCH):

            @pl.when(b == NCH + 2 * j)
            def _():
                if j == 0:
                    first_x.wait_recv()
                own_x(j).wait_recv()
                x_other(j).start()
                x_on(j).start()
                if j == 0:
                    first_y.wait_recv()
                own_y(j).wait_recv()
                y_other(j).start()
                y_on(j).start()
                x_other(j).wait_recv()

            @pl.when(b == NCH + 2 * j + 1)
            def _():
                y_other(j).wait_recv()

        @pl.when(b == 3 * NCH)
        def _():
            pass_on(0)
            d_other(0).wait_recv()

        project_rows(2 * b, 2)

    def project_rows(p0, count):
        rows = xg[pl.ds(pl.multiple_of(p0 * CH, CH), count * CH), :]
        places, trig = [], []
        for i in range(count):
            at = chunk_of(p0 + i)
            places.append(pl.ds(pl.multiple_of(at * CH, CH), CH))
            cf, sf = far_v[0, pl.ds(at, 1), :], far_v[1, pl.ds(at, 1), :]
            cn, sn = near_v[0], near_v[1]
            trig.append((cf * cn - sf * sn, sf * cn + cf * sn))
        for n, to in ((0, q), (1, k)):
            for h in range(2):
                t = dot(rows, w[n, :, h * HEAD : (h + 1) * HEAD]).astype(bf16).astype(f32)
                for i in range(count):
                    a, b_ = t[i * CH : (i + 1) * CH, : HEAD // 2], t[i * CH : (i + 1) * CH, HEAD // 2 :]
                    cos, sin = trig[i]
                    to[h, places[i], :] = jnp.concatenate([a * cos - b_ * sin, b_ * cos + a * sin], -1).astype(bf16)
        for h in range(2):
            t = dot(rows, w[2, :, h * HEAD : (h + 1) * HEAD]).astype(bf16)
            for i in range(count):
                vt[h, 0:HEAD, places[i]] = t[i * CH : (i + 1) * CH].T

    def place(i):
        return pl.ds(pl.multiple_of(i * WIDTH, WIDTH), WIDTH)

    def attention(i, to, strips=range(NS)):
        pieces = [(h, s) for h in range(2) for s in strips]
        q0 = pl.multiple_of(to * CHIP, CHIP)
        for n in range(len(pieces)):
            top_s[n : n + 1, :] = jnp.full((1, STRIP), NEG, f32)
            mix_s[n] = jnp.zeros(mix_s.shape[1:], f32)

        def block(k0, masked):
            def score(n):
                h, s = pieces[n]
                keys = (s + 1) * STRIP if masked else CHIP
                return dot(k[h, pl.ds(k0, keys), :], q[h, pl.ds(q0 + s * STRIP, STRIP), :], 1, 1)

            def soften(n, sc):
                s = pieces[n][1]
                if masked:
                    ok = (lax.broadcasted_iota(jnp.int32, sc.shape, 0) - s * STRIP) <= lax.broadcasted_iota(jnp.int32, sc.shape, 1)
                    sc = jnp.where(ok, sc, 2 * NEG)
                old = top_s[n : n + 1, :]
                top = jnp.maximum(old, sc.max(axis=0, keepdims=True))
                top_s[n : n + 1, :] = top
                return jnp.exp2((sc - top) * E2).astype(bf16), jnp.exp2((old - top) * E2)

            def mix(n, p, keep):
                h, s = pieces[n]
                keys = (s + 1) * STRIP if masked else CHIP
                mix_s[n] = mix_s[n] * keep + dot(vt[h, :, pl.ds(k0, keys)], p)

            count = len(pieces)
            scores = {n: score(n) for n in range(min(AHEAD, count))}
            held = None
            for n in range(count):
                soft = soften(n, scores.pop(n))
                if held is not None:
                    mix(n - 1, *held)
                held = soft
                if n + AHEAD < count:
                    scores[n + AHEAD] = score(n + AHEAD)
            mix(count - 1, *held)

        lax.fori_loop(0, to, lambda j, _: block(pl.multiple_of(j * CHIP, CHIP), False), None)
        block(q0, True)
        for n, (h, s) in enumerate(pieces):
            out = mix_s[n, 0:HEAD, :] * (1 / mix_s[n, HEAD : HEAD + 1, :])
            xg[s * STRIP : (s + 1) * STRIP, pl.ds(pl.multiple_of(i * WIDTH + h * HEAD, HEAD), HEAD)] = out.T.astype(bf16)

    def part(of, p):
        return pl.ds(pl.multiple_of(jnp.where(p == 0, of * CH, (1 - of) * STRIP), CH), CH if p else STRIP)

    def results(of, p=None):
        if p is None:
            return pl.ds(pl.multiple_of(of * ROWS, ROWS), ROWS)
        rows = part(of, p)
        return pl.ds(pl.multiple_of(of * ROWS + rows.start, CH), rows.size)

    def exchange(i):
        return remote(xg.at[results(1 - core), place(i)], pb.at[i], ex_s.at[5], ex_s.at[i], other)

    def exchange_part(p):
        slot = 4 if p else 2
        return remote(xg.at[results(1 - core, p), place(2)], pb.at[2, part(1 - core, p)], ex_s.at[5], ex_s.at[slot], other)

    def term(i, t, p=None):
        mine = xg[results(core, p), place(i)]
        theirs = pb[i] if p is None else pb[i, part(core, p)]
        return dot(jnp.concatenate([mine, theirs], axis=1), wo[:, cols(t)])

    def cols(t):
        return pl.ds(pl.multiple_of(t * TILE, TILE), TILE)

    SX, SY, SD = (slice(n * ROWS, (n + 1) * ROWS) for n in range(2, 5))
    SUMS_IN = slice(5 * ROWS, 6 * ROWS)
    RD, DIR = (slice(n * ROWS, (n + 1) * ROWS) for n in range(6, 8))
    lxr = pltpu.make_async_copy(x_ref, o_ref, load.at[0])

    def send_xd(t):
        return remote(xg.at[SX, cols(t)], direct_h.at[:, cols(t)], rs_s.at[0], rs_r.at[2 * HT], dev_x)

    def send_yd(t):
        rows, at = pl.ds(pl.multiple_of(t // 2 * ROWS, ROWS), ROWS), cols(4 + lax.rem(t, 2))
        return remote(xg.at[rows, at], direct_h.at[:, cols(HT + t)], rs_s.at[0], rs_r.at[2 * HT], dev_y)

    def send_x(t):
        return remote(xg.at[SX, cols(HT + t)], xg.at[SUMS_IN, cols(HT + t)], rs_s.at[0], rs_r.at[HT + t], dev_x)

    def send_y(t):
        return remote(xg.at[SY, cols(t)], xg.at[SUMS_IN, cols(t)], rs_s.at[0], rs_r.at[t], dev_y)

    def fetch_d(t):
        return pltpu.make_async_copy(diag_h.at[:, cols(t)], xg.at[RD, cols(t)], fetch.at[0])

    fetch_direct = pltpu.make_async_copy(direct_h, xg.at[DIR], fetch.at[1])

    def staged(p):
        rows = part(core, p)
        return pl.ds(pl.multiple_of(SD.start + rows.start, CH), rows.size)

    def send_d(t, p):
        return remote(xg.at[staged(p), cols(t)], diag_h.at[part(core, p), cols(t)], rs_s.at[0], rs_r.at[2 * HT + 1 + t], dev_x)

    def send_e(t, p):
        return remote(xg.at[staged(p), cols(t)], diag_h.at[part(core, p), cols(t)], rs_s.at[0], rs_r.at[2 * HT + 1 + t], dev_y)

    def diagonal(p):
        lax.fori_loop(0, HT, functools.partial(diagonal_pieces, p), None)

    def diagonal_pieces(p, t, _):
        rows = staged(p)
        xg[rows, cols(t)] = term(2, t, p).astype(bf16)
        send_d(t, p).start()
        xg[rows, cols(HT + t)] = term(2, HT + t, p).astype(bf16)
        send_e(HT + t, p).start()

    def item(n):
        x_first = chip_x < chip_y
        to = jnp.where(n == 2, chip, jnp.where((n == 0) == x_first, chip_x, chip_y))
        i = jnp.where(n == 2, 3, jnp.where((n == 0) == x_first, 0, 1))
        attention(i, to)
        ex = exchange(i)
        ex.start()

        @pl.when(n == 0)
        def _():
            sent(3 * CH, fwd_s.at[0])

        ex.wait_recv()

        def direct(t, _):
            tx, ty = t, HT + t

            @pl.when(i == 0)
            def _():
                xg[SX, cols(tx)] = term(0, tx).astype(bf16)
                send_xd(t).start()

            @pl.when(i == 1)
            def _():
                xg[pl.ds(pl.multiple_of(t // 2 * ROWS, ROWS), ROWS), cols(4 + lax.rem(t, 2))] = term(1, ty).astype(bf16)
                send_yd(t).start()

        lax.fori_loop(0, jnp.where(i == 3, 0, HT), direct, None)

    early = jnp.where(chip == 0, 2, jnp.where(chip == 3, 0, 1))
    first = 3 * NCH
    late = first + 3

    def step(n, _):
        @pl.when(n == first)
        def _():
            lwo.wait()
            wo_copy.wait()
            sent(3 * ROWS, own_s.at[0])

        m = n - early
        is_item = ((n >= first) & (n < first + early)) | (m >= late)
        on = (n < first) | (m >= first)

        @pl.when((n < first) | (on & (m == first)))
        def _():
            project(jnp.where(n < first, n, first))

        def diagonal_rows(j, of):
            @pl.when(core != of)
            def _():
                d_other(j).wait_recv()

            project_rows(diag(j, jnp.where(core == of, 0, 1)), 1)

        @pl.when(on & (m == first + 1))
        def _():
            pass_on(1)
            diagonal_rows(1, 0)
            attention(2, chip_d, range(1))

            @pl.when(core == 1)
            def _():
                exchange_part(0).start()

            diagonal_rows(1, 1)
            sent(3 * CH, fwd_s.at[1])

            @pl.when(core == 0)
            def _():
                exchange_part(0).wait_recv()
                diagonal_pieces(0, 0, None)

            pass_on(2)
            sent(3 * CH, fwd_s.at[2])
            lxr.start()

            @pl.when(core == 0)
            def _():
                lax.fori_loop(1, HT, functools.partial(diagonal_pieces, 0), None)

        @pl.when(on & (m == first + 2))
        def _():
            diagonal_rows(2, 0)
            attention(2, chip_d, range(1, 2))
            exchange_part(1).start()
            diagonal_rows(2, 1)
            at_once = (core == 0) & (chip != 3)

            @pl.when(at_once)
            def _():
                exchange_part(1).wait_recv()
                diagonal(1)

            for to in (dev_x, dev_y):
                pl.semaphore_signal(free, inc=1, device_id={"tp": to}, device_id_type=pl.DeviceIdType.MESH)
            sent(NCH * CH, fwd_s.at[NCH])
            attention(2, chip_d, range(2, 3))

            @pl.when(core == 0)
            def _():
                exchange_part(0).start()

            @pl.when(jnp.logical_not(at_once))
            def _():
                exchange_part(1).wait_recv()
                diagonal(1)

            @pl.when(core == 1)
            def _():
                exchange_part(0).wait_recv()
                diagonal(0)

        @pl.when(is_item)
        def _():
            item(jnp.where(n < first + early, n - first, m - late + early))

    lax.fori_loop(0, late + 3, step, None)

    def diagonal_in(t):
        remote(xg.at[SD, cols(t)], diag_h.at[:, cols(t)], rs_s.at[0], rs_r.at[2 * HT + 1 + t], dev_x).wait_recv()

    def combine(t, _):
        tx, ty = HT + t, t
        diagonal_in(tx)
        fetch_d(tx).start()
        fetch_d(tx).wait()
        xg[SX, cols(tx)] = (term(0, tx) + xg[RD, cols(tx)].astype(f32)).astype(bf16)
        send_x(t).start()
        diagonal_in(ty)
        fetch_d(ty).start()
        fetch_d(ty).wait()
        xg[SY, cols(ty)] = (term(1, ty) + xg[RD, cols(ty)].astype(f32)).astype(bf16)
        send_y(t).start()

    pl.semaphore_wait(free, 2)
    lax.fori_loop(0, HT, combine, None)

    remote(xg.at[SX], direct_h, rs_s.at[0], rs_r.at[2 * HT], dev_x).wait_recv()
    fetch_direct.start()
    lxr.wait()
    fetch_direct.wait()

    def finish(t, _):
        def known(t):
            return o_ref[:, cols(t)].astype(f32) + (term(3, t) + xg[DIR, cols(t)].astype(f32))

        def add(t, total):
            o_ref[:, cols(t)] = (total + xg[SUMS_IN, cols(t)].astype(f32)).astype(bf16)

        left, right = known(t), known(HT + t)
        send_y(t).wait_recv()
        add(t, left)
        send_x(t).wait_recv()
        add(HT + t, right)

    lax.fori_loop(0, HT, finish, None)
    sent(3 * ROWS, rs_s.at[0])
    remote(pb, pb, ex_s.at[5], ex_s.at[0], other).wait_send()


def in_hbm(a):
    return pltpu.with_memory_space_constraint(jnp.asarray(a), pltpu.HBM)


def solution(mesh):
    def step(x, gain, wq, wk, wv, wo):
        rate = THETA ** (-np.arange(HEAD // 2) / (HEAD // 2))
        near = np.arange(CH)[:, None] * rate
        far = (np.arange(SEQ // CH) * CH)[:, None] * rate
        near, far = (np.stack([np.cos(a), np.sin(a)]).astype(np.float32) for a in (near, far))
        hbm = pl.BlockSpec(memory_space=pltpu.HBM)
        dma, V = pltpu.SemaphoreType.DMA, pltpu.VMEM
        return pl.pallas_call(
            kernel,
            out_shape=[jax.ShapeDtypeStruct((ROWS, D), bf16)] * 3,
            in_specs=[hbm] * 8,
            out_specs=[pl.BlockSpec(memory_space=pltpu.VMEM), hbm, hbm],
            scratch_shapes=[
                V((SEQ, D), bf16),
                V((3, D, WIDTH), bf16),
                V((2 * WIDTH, D), bf16),
                V((2, SEQ, HEAD), bf16),
                V((2, SEQ, HEAD), bf16),
                V((2, HEAD + SUMS, SEQ), bf16),
                V((4, ROWS, WIDTH), bf16),
                V((8, STRIP), f32),
                V((2 * NS, HEAD + SUMS, STRIP), f32),
                V((D,), bf16), V(near.shape, f32), V(far.shape, f32),
                dma((6 + NCH,)), dma((1,)), dma((3, NCH + 1)), dma((NCH + 1,)), dma((5, NCH)), dma((2,)), dma((6,)),
                dma((1,)), dma((4 * HT + 1,)), dma((2,)), pltpu.SemaphoreType.REGULAR,
            ],
            compiler_params=pltpu.CompilerParams(collective_id=0, has_side_effects=True, vmem_limit_bytes=53_900_000),
        )(x, in_hbm(gain), wq, wk, wv, wo, in_hbm(near), in_hbm(far))[0]

    tokens, columns = P(("dp", "tp"), None), P(None, "tp")
    return jax.shard_map(
        step,
        mesh=mesh,
        in_specs=(tokens, P(None), columns, columns, columns, P("tp", None)),
        out_specs=tokens,
        check_vma=False,
    )
```

```python
import functools

import jax
import jax.numpy as jnp
import numpy as np
from jax import lax
from jax.experimental import pallas as pl
from jax.experimental.pallas import tpu as pltpu
from jax.sharding import PartitionSpec as P

HEAD = 256
THETA = 10000
LOG2E = 1.4426950408889634
NEG = -1e30
EPS = 1e-6
CH = 128
NCH = 3
SUB = 32
ROWS = CH * NCH
D = 3072
HALF = D // 2
TILE = 512
HT = HALF // TILE
SEQ = 8 * ROWS
CHIP = 2 * ROWS
STRIP = 256
NS = CHIP // STRIP
AHEAD = 3
SUMS = 8
WIDTH = 2 * HEAD
SCALE = HEAD**-0.5
E2 = SCALE * LOG2E

f32, bf16 = jnp.float32, jnp.bfloat16


def dot(a, b, ca=1, cb=0):
    return lax.dot_general(a, b, (((ca,), (cb,)), ((), ())), preferred_element_type=f32)


def kernel(x_ref, gain_ref, wq_ref, wk_ref, wv_ref, wo_ref, near_ref, far_ref, o_ref, diag_h, direct_h,
           xg, w, wo, q, k, vt, pb, top_s, mix_s, gain_v, near_v, far_v,
           load, own_s, arr, fwd_s, arr2, wo_s, ex_s, rs_s, rs_r, fetch, free):
    me = lax.axis_index("tp")
    chip = me // 2
    core = me - 2 * chip
    chip_x = lax.rem(chip + 2, 4)
    chip_y = chip + 1 - 2 * lax.rem(chip, 2)
    chip_d = 3 - chip
    other, dev_x, dev_y = 2 * chip + 1 - core, 2 * chip_x + core, 2 * chip_y + core

    def remote(src, dst, s, r, to):
        return pltpu.make_async_remote_copy(src_ref=src, dst_ref=dst, send_sem=s, recv_sem=r, device_id={"tp": to},
                                            device_id_type=pl.DeviceIdType.MESH)

    def piece(p):
        return pl.ds(pl.multiple_of(p * CH, CH), CH)

    lgain = pltpu.make_async_copy(gain_ref, gain_v, load.at[3])
    lgain.start()
    lx0 = pltpu.make_async_copy(x_ref.at[pl.ds(0, SUB)], vt.at[0, 0:SUB], load.at[6 + NCH])
    lxs = []
    for j in range(NCH):
        skip = 0 if j else SUB
        lxs.append(pltpu.make_async_copy(x_ref.at[pl.ds(j * CH + skip, CH - skip)],
                                         vt.at[j // 2, j % 2 * CH + skip : (j % 2 + 1) * CH], load.at[6 + j]))
    lx0.start()
    for c in lxs:
        c.start()
    lnear, lfar = pltpu.make_async_copy(near_ref, near_v, load.at[4]), pltpu.make_async_copy(far_ref, far_v, load.at[5])
    lnear.start()
    lfar.start()
    lws = [pltpu.make_async_copy(r, w.at[i], load.at[1]) for i, r in enumerate((wq_ref, wk_ref, wv_ref))]
    for c in lws:
        c.start()
    lwo = pltpu.make_async_copy(wo_ref, wo.at[0:WIDTH], load.at[2])
    lwo.start()

    barrier = pltpu.get_barrier_semaphore()
    for to in (other, dev_x, dev_y):
        pl.semaphore_signal(barrier, inc=1, device_id={"tp": to}, device_id_type=pl.DeviceIdType.MESH)
    lgain.wait()
    lx0.wait()

    def nbr(j, i):
        return 2 * NCH + 4 * j + i

    def diag(j, i):
        return 6 * NCH + 2 * j + i

    def sent(rows, s):
        remote(xg.at[0:rows], xg.at[0:rows], s, wo_s.at[1], other).wait_send()

    def own_other(j):
        return remote(xg.at[piece(j)], xg.at[piece(NCH + j)], own_s.at[0], arr.at[0, j], other)

    def own_rest(j, at, r, to):
        skip = 0 if j else SUB
        return remote(xg.at[pl.ds(j * CH + skip, CH - skip)], xg.at[pl.ds(nbr(j, at) * CH + skip, CH - skip)], own_s.at[0], r, to)

    def own_first(at, r, to):
        return remote(xg.at[pl.ds(0, SUB)], xg.at[pl.ds(nbr(0, at) * CH, SUB)], own_s.at[0], r, to)

    def came(j, at, r):
        remote(xg.at[piece(j)], xg.at[piece(nbr(j, at))], own_s.at[0], r, dev_x).wait_recv()

    def own_x(j):
        return own_rest(j, 0, arr.at[1, j], dev_x)

    def own_y(j):
        return own_rest(j, 2, arr.at[2, j], dev_y)

    first_x, first_y = own_first(0, arr.at[1, 0], dev_x), own_first(2, arr.at[2, 0], dev_y)

    def x_other(j):
        return remote(xg.at[piece(nbr(j, 0))], xg.at[piece(nbr(j, 1))], fwd_s.at[j], arr2.at[0, j], other)

    def y_other(j):
        return remote(xg.at[piece(nbr(j, 2))], xg.at[piece(nbr(j, 3))], fwd_s.at[j], arr2.at[1, j], other)

    def x_on(j):
        return remote(xg.at[piece(nbr(j, 0)), 0:HALF], xg.at[piece(diag(j, 0)), 0:HALF], fwd_s.at[j], arr2.at[2, j], dev_y)

    def y_on(j):
        return remote(xg.at[piece(nbr(j, 2)), HALF:D], xg.at[piece(diag(j, 0)), HALF:D], fwd_s.at[j], arr2.at[2, j], dev_x)

    def d_other(j):
        return remote(xg.at[piece(diag(j, 0))], xg.at[piece(diag(j, 1))], fwd_s.at[NCH], arr2.at[3, j], other)

    def pass_on(j):
        remote(xg.at[piece(diag(j, 0))], xg.at[piece(diag(j, 0))], own_s.at[0], arr2.at[2, j], dev_y).wait_recv()
        d_other(j).start()

    gain = gain_v[...].reshape(1, D).astype(f32)
    per = CH // SUB

    def norm(i, _):
        rows = pl.ds(pl.multiple_of(i * SUB, SUB), SUB)
        p = i // per
        wide = vt[p // 2, pl.ds(pl.multiple_of(lax.rem(p, 2) * CH + lax.rem(i, per) * SUB, SUB), SUB), :].astype(f32)
        scale = lax.rsqrt(jnp.mean(wide * wide, -1, keepdims=True) + EPS)
        xg[rows, :] = (wide * scale * gain).astype(bf16)

    norm(0, None)
    pl.semaphore_wait(barrier, 3)
    first_x.start()
    first_y.start()
    lxs[0].wait()
    lax.fori_loop(1, per, norm, None)
    for j in range(NCH):
        own_x(j).start()
        own_y(j).start()
        own_other(j).start()
        if j + 1 < NCH:
            lxs[j + 1].wait()
            lax.fori_loop((j + 1) * per, (j + 2) * per, norm, None)
    wo_copy = remote(wo_ref, wo.at[WIDTH : 2 * WIDTH], wo_s.at[0], wo_s.at[1], other)
    wo_copy.start()
    for h in range(2):
        vt[h, HEAD : HEAD + SUMS, :] = jnp.ones((SUMS, SEQ), bf16)
    pltpu.make_async_copy(w, w, load.at[1]).wait()
    lnear.wait()
    lfar.wait()

    def chunk_of(p):
        mine, theirs = 2 * chip + core, 2 * chip + 1 - core
        n = jnp.maximum(p - 2 * NCH, 0)
        nj, ni = n // 4, lax.rem(n, 4)
        nd = 2 * jnp.where(ni < 2, chip_x, chip_y) + jnp.where(lax.rem(ni, 2) == 0, core, 1 - core)
        m = jnp.maximum(p - 6 * NCH, 0)
        mj, mi = m // 2, lax.rem(m, 2)
        md = 2 * chip_d + jnp.where(mi == 0, core, 1 - core)
        at = jnp.where(p < NCH, mine * NCH + p, theirs * NCH + p - NCH)
        at = jnp.where(p >= 2 * NCH, nd * NCH + nj, at)
        return jnp.where(p >= 6 * NCH, md * NCH + mj, at)

    def project(b):
        @pl.when(b == 1)
        def _():
            own_other(0).wait_recv()

        @pl.when(b == 2)
        def _():
            own_other(1).wait_recv()
            own_other(2).wait_recv()

        for j in range(NCH):

            @pl.when(b == NCH + 2 * j)
            def _():
                came(j, 0, arr.at[1, j])
                x_other(j).start()
                x_on(j).start()
                came(j, 2, arr.at[2, j])
                y_other(j).start()
                y_on(j).start()
                x_other(j).wait_recv()

            @pl.when(b == NCH + 2 * j + 1)
            def _():
                y_other(j).wait_recv()

        @pl.when(b == 3 * NCH)
        def _():
            pass_on(0)
            d_other(0).wait_recv()

        project_rows(2 * b, 2)

    def project_rows(p0, count):
        rows = xg[pl.ds(pl.multiple_of(p0 * CH, CH), count * CH), :]
        places, trig = [], []
        for i in range(count):
            at = chunk_of(p0 + i)
            places.append(pl.ds(pl.multiple_of(at * CH, CH), CH))
            cf, sf = far_v[0, pl.ds(at, 1), :], far_v[1, pl.ds(at, 1), :]
            cn, sn = near_v[0], near_v[1]
            trig.append((cf * cn - sf * sn, sf * cn + cf * sn))
        for n, to in ((0, q), (1, k)):
            for h in range(2):
                t = dot(rows, w[n, :, h * HEAD : (h + 1) * HEAD]).astype(bf16).astype(f32)
                for i in range(count):
                    a, b_ = t[i * CH : (i + 1) * CH, : HEAD // 2], t[i * CH : (i + 1) * CH, HEAD // 2 :]
                    cos, sin = trig[i]
                    to[h, places[i], :] = jnp.concatenate([a * cos - b_ * sin, b_ * cos + a * sin], -1).astype(bf16)
        for h in range(2):
            t = dot(rows, w[2, :, h * HEAD : (h + 1) * HEAD]).astype(bf16)
            for i in range(count):
                vt[h, 0:HEAD, places[i]] = t[i * CH : (i + 1) * CH].T

    def place(i):
        return pl.ds(pl.multiple_of(i * WIDTH, WIDTH), WIDTH)

    def attention(i, to, strips=range(NS)):
        pieces = [(h, s) for h in range(2) for s in strips]
        q0 = pl.multiple_of(to * CHIP, CHIP)
        for n in range(len(pieces)):
            top_s[n : n + 1, :] = jnp.full((1, STRIP), NEG, f32)
            mix_s[n] = jnp.zeros(mix_s.shape[1:], f32)

        def block(k0, masked):
            def score(n):
                h, s = pieces[n]
                keys = (s + 1) * STRIP if masked else CHIP
                return dot(k[h, pl.ds(k0, keys), :], q[h, pl.ds(q0 + s * STRIP, STRIP), :], 1, 1)

            def soften(n, sc):
                s = pieces[n][1]
                if masked:
                    ok = (lax.broadcasted_iota(jnp.int32, sc.shape, 0) - s * STRIP) <= lax.broadcasted_iota(jnp.int32, sc.shape, 1)
                    sc = jnp.where(ok, sc, 2 * NEG)
                old = top_s[n : n + 1, :]
                top = jnp.maximum(old, sc.max(axis=0, keepdims=True))
                top_s[n : n + 1, :] = top
                return jnp.exp2((sc - top) * E2).astype(bf16), jnp.exp2((old - top) * E2)

            def mix(n, p, keep):
                h, s = pieces[n]
                keys = (s + 1) * STRIP if masked else CHIP
                mix_s[n] = mix_s[n] * keep + dot(vt[h, :, pl.ds(k0, keys)], p)

            count = len(pieces)
            scores = {n: score(n) for n in range(min(AHEAD, count))}
            held = None
            for n in range(count):
                soft = soften(n, scores.pop(n))
                if held is not None:
                    mix(n - 1, *held)
                held = soft
                if n + AHEAD < count:
                    scores[n + AHEAD] = score(n + AHEAD)
            mix(count - 1, *held)

        lax.fori_loop(0, to, lambda j, _: block(pl.multiple_of(j * CHIP, CHIP), False), None)
        block(q0, True)
        for n, (h, s) in enumerate(pieces):
            out = mix_s[n, 0:HEAD, :] * (1 / mix_s[n, HEAD : HEAD + 1, :])
            xg[s * STRIP : (s + 1) * STRIP, pl.ds(pl.multiple_of(i * WIDTH + h * HEAD, HEAD), HEAD)] = out.T.astype(bf16)

    def part(of, p):
        return pl.ds(pl.multiple_of(jnp.where(p == 0, of * CH, (1 - of) * STRIP), CH), CH if p else STRIP)

    def results(of, p=None):
        if p is None:
            return pl.ds(pl.multiple_of(of * ROWS, ROWS), ROWS)
        rows = part(of, p)
        return pl.ds(pl.multiple_of(of * ROWS + rows.start, CH), rows.size)

    def exchange(i):
        return remote(xg.at[results(1 - core), place(i)], pb.at[i], ex_s.at[5], ex_s.at[i], other)

    def exchange_part(p):
        slot = 4 if p else 2
        return remote(xg.at[results(1 - core, p), place(2)], pb.at[2, part(1 - core, p)], ex_s.at[5], ex_s.at[slot], other)

    def term(i, t, p=None):
        mine = xg[results(core, p), place(i)]
        theirs = pb[i] if p is None else pb[i, part(core, p)]
        return dot(jnp.concatenate([mine, theirs], axis=1), wo[:, cols(t)])

    def cols(t):
        return pl.ds(pl.multiple_of(t * TILE, TILE), TILE)

    SX, SY, SD = (slice(n * ROWS, (n + 1) * ROWS) for n in range(2, 5))
    SUMS_IN = slice(5 * ROWS, 6 * ROWS)
    RD, DIR = (slice(n * ROWS, (n + 1) * ROWS) for n in range(6, 8))
    lxr = pltpu.make_async_copy(x_ref, o_ref, load.at[0])

    def send_xd(t):
        return remote(xg.at[SX, cols(t)], direct_h.at[:, cols(t)], rs_s.at[0], rs_r.at[2 * HT], dev_x)

    def send_yd(t):
        rows, at = pl.ds(pl.multiple_of(t // 2 * ROWS, ROWS), ROWS), cols(4 + lax.rem(t, 2))
        return remote(xg.at[rows, at], direct_h.at[:, cols(HT + t)], rs_s.at[0], rs_r.at[2 * HT], dev_y)

    def send_x(t):
        return remote(xg.at[SX, cols(HT + t)], xg.at[SUMS_IN, cols(HT + t)], rs_s.at[0], rs_r.at[HT + t], dev_x)

    def send_y(t):
        return remote(xg.at[SY, cols(t)], xg.at[SUMS_IN, cols(t)], rs_s.at[0], rs_r.at[t], dev_y)

    def fetch_d(t):
        return pltpu.make_async_copy(diag_h.at[:, cols(t)], xg.at[RD, cols(t)], fetch.at[0])

    fetch_direct = pltpu.make_async_copy(direct_h, xg.at[DIR], fetch.at[1])

    def staged(p):
        rows = part(core, p)
        return pl.ds(pl.multiple_of(SD.start + rows.start, CH), rows.size)

    def send_d(t, p):
        return remote(xg.at[staged(p), cols(t)], diag_h.at[part(core, p), cols(t)], rs_s.at[0], rs_r.at[2 * HT + 1 + t], dev_x)

    def send_e(t, p):
        return remote(xg.at[staged(p), cols(t)], diag_h.at[part(core, p), cols(t)], rs_s.at[0], rs_r.at[2 * HT + 1 + t], dev_y)

    def diagonal(p):
        lax.fori_loop(0, HT, functools.partial(diagonal_pieces, p), None)

    def diagonal_pieces(p, t, _):
        rows = staged(p)
        xg[rows, cols(t)] = term(2, t, p).astype(bf16)
        send_d(t, p).start()
        xg[rows, cols(HT + t)] = term(2, HT + t, p).astype(bf16)
        send_e(HT + t, p).start()

    def item(n):
        x_first = chip_x < chip_y
        to = jnp.where(n == 2, chip, jnp.where((n == 0) == x_first, chip_x, chip_y))
        i = jnp.where(n == 2, 3, jnp.where((n == 0) == x_first, 0, 1))
        attention(i, to)
        ex = exchange(i)
        ex.start()

        @pl.when(n == 0)
        def _():
            sent(3 * CH, fwd_s.at[0])

        ex.wait_recv()

        def direct(t, _):
            tx, ty = t, HT + t

            @pl.when(i == 0)
            def _():
                xg[SX, cols(tx)] = term(0, tx).astype(bf16)
                send_xd(t).start()

            @pl.when(i == 1)
            def _():
                xg[pl.ds(pl.multiple_of(t // 2 * ROWS, ROWS), ROWS), cols(4 + lax.rem(t, 2))] = term(1, ty).astype(bf16)
                send_yd(t).start()

        lax.fori_loop(0, jnp.where(i == 3, 0, HT), direct, None)

    early = jnp.where(chip == 0, 2, jnp.where(chip == 3, 0, 1))
    first = 3 * NCH
    late = first + 3

    def step(n, _):
        @pl.when(n == first)
        def _():
            lwo.wait()
            wo_copy.wait()
            sent(3 * ROWS, own_s.at[0])

        m = n - early
        is_item = ((n >= first) & (n < first + early)) | (m >= late)
        on = (n < first) | (m >= first)

        @pl.when((n < first) | (on & (m == first)))
        def _():
            project(jnp.where(n < first, n, first))

        def diagonal_rows(j, of):
            @pl.when(core != of)
            def _():
                d_other(j).wait_recv()

            project_rows(diag(j, jnp.where(core == of, 0, 1)), 1)

        @pl.when(on & (m == first + 1))
        def _():
            pass_on(1)
            diagonal_rows(1, 0)
            attention(2, chip_d, range(1))

            @pl.when(core == 1)
            def _():
                exchange_part(0).start()

            diagonal_rows(1, 1)
            sent(3 * CH, fwd_s.at[1])

            @pl.when(core == 0)
            def _():
                exchange_part(0).wait_recv()
                diagonal_pieces(0, 0, None)

            pass_on(2)
            sent(3 * CH, fwd_s.at[2])
            lxr.start()

            @pl.when(core == 0)
            def _():
                lax.fori_loop(1, HT, functools.partial(diagonal_pieces, 0), None)

        @pl.when(on & (m == first + 2))
        def _():
            diagonal_rows(2, 0)
            attention(2, chip_d, range(1, 2))
            exchange_part(1).start()
            diagonal_rows(2, 1)
            at_once = (core == 0) & (chip != 3)

            @pl.when(at_once)
            def _():
                exchange_part(1).wait_recv()
                diagonal(1)

            for to in (dev_x, dev_y):
                pl.semaphore_signal(free, inc=1, device_id={"tp": to}, device_id_type=pl.DeviceIdType.MESH)
            sent(NCH * CH, fwd_s.at[NCH])
            attention(2, chip_d, range(2, 3))

            @pl.when(core == 0)
            def _():
                exchange_part(0).start()

            @pl.when(jnp.logical_not(at_once))
            def _():
                exchange_part(1).wait_recv()
                diagonal(1)

            @pl.when(core == 1)
            def _():
                exchange_part(0).wait_recv()
                diagonal(0)

        @pl.when(is_item)
        def _():
            item(jnp.where(n < first + early, n - first, m - late + early))

    lax.fori_loop(0, late + 3, step, None)

    def diagonal_in(t):
        remote(xg.at[SD, cols(t)], diag_h.at[:, cols(t)], rs_s.at[0], rs_r.at[2 * HT + 1 + t], dev_x).wait_recv()

    def combine(t, _):
        tx, ty = HT + t, t
        diagonal_in(tx)
        fetch_d(tx).start()
        fetch_d(tx).wait()
        xg[SX, cols(tx)] = (term(0, tx) + xg[RD, cols(tx)].astype(f32)).astype(bf16)
        send_x(t).start()
        diagonal_in(ty)
        fetch_d(ty).start()
        fetch_d(ty).wait()
        xg[SY, cols(ty)] = (term(1, ty) + xg[RD, cols(ty)].astype(f32)).astype(bf16)
        send_y(t).start()

    pl.semaphore_wait(free, 2)
    lax.fori_loop(0, HT, combine, None)

    remote(xg.at[SX], direct_h, rs_s.at[0], rs_r.at[2 * HT], dev_x).wait_recv()
    fetch_direct.start()
    lxr.wait()
    fetch_direct.wait()

    def finish(t, _):
        def known(t):
            return o_ref[:, cols(t)].astype(f32) + (term(3, t) + xg[DIR, cols(t)].astype(f32))

        def add(t, total):
            o_ref[:, cols(t)] = (total + xg[SUMS_IN, cols(t)].astype(f32)).astype(bf16)

        left, right = known(t), known(HT + t)
        send_y(t).wait_recv()
        add(t, left)
        send_x(t).wait_recv()
        add(HT + t, right)

    lax.fori_loop(0, HT, finish, None)
    sent(3 * ROWS, rs_s.at[0])
    remote(pb, pb, ex_s.at[5], ex_s.at[0], other).wait_send()


def in_hbm(a):
    return pltpu.with_memory_space_constraint(jnp.asarray(a), pltpu.HBM)


def solution(mesh):
    def step(x, gain, wq, wk, wv, wo):
        rate = THETA ** (-np.arange(HEAD // 2) / (HEAD // 2))
        near = np.arange(CH)[:, None] * rate
        far = (np.arange(SEQ // CH) * CH)[:, None] * rate
        near, far = (np.stack([np.cos(a), np.sin(a)]).astype(np.float32) for a in (near, far))
        hbm = pl.BlockSpec(memory_space=pltpu.HBM)
        dma, V = pltpu.SemaphoreType.DMA, pltpu.VMEM
        return pl.pallas_call(
            kernel,
            out_shape=[jax.ShapeDtypeStruct((ROWS, D), bf16)] * 3,
            in_specs=[hbm] * 8,
            out_specs=[pl.BlockSpec(memory_space=pltpu.VMEM), hbm, hbm],
            scratch_shapes=[
                V((SEQ, D), bf16),
                V((3, D, WIDTH), bf16),
                V((2 * WIDTH, D), bf16),
                V((2, SEQ, HEAD), bf16),
                V((2, SEQ, HEAD), bf16),
                V((2, HEAD + SUMS, SEQ), bf16),
                V((4, ROWS, WIDTH), bf16),
                V((8, STRIP), f32),
                V((2 * NS, HEAD + SUMS, STRIP), f32),
                V((D,), bf16), V(near.shape, f32), V(far.shape, f32),
                dma((7 + NCH,)), dma((1,)), dma((3, NCH)), dma((NCH + 1,)), dma((4, NCH)), dma((2,)), dma((6,)),
                dma((1,)), dma((4 * HT + 1,)), dma((2,)), pltpu.SemaphoreType.REGULAR,
            ],
            compiler_params=pltpu.CompilerParams(collective_id=0, has_side_effects=True, vmem_limit_bytes=53_900_000),
        )(x, in_hbm(gain), wq, wk, wv, wo, in_hbm(near), in_hbm(far))[0]

    tokens, columns = P(("dp", "tp"), None), P(None, "tp")
    return jax.shard_map(
        step,
        mesh=mesh,
        in_specs=(tokens, P(None), columns, columns, columns, P("tp", None)),
        out_specs=tokens,
        check_vma=False,
    )
```

```python
import functools

import jax
import jax.numpy as jnp
import numpy as np
from jax import lax
from jax.experimental import pallas as pl
from jax.experimental.pallas import tpu as pltpu
from jax.sharding import PartitionSpec as P

HEAD = 256
THETA = 10000
LOG2E = 1.4426950408889634
NEG = -1e30
EPS = 1e-6
CH = 128
NCH = 3
SUB = 32
ROWS = CH * NCH
D = 3072
HALF = D // 2
TILE = 512
HT = HALF // TILE
SEQ = 8 * ROWS
CHIP = 2 * ROWS
STRIP = 256
NS = CHIP // STRIP
AHEAD = 3
SUMS = 8
WIDTH = 2 * HEAD
SCALE = HEAD**-0.5
E2 = SCALE * LOG2E

f32, bf16 = jnp.float32, jnp.bfloat16


def dot(a, b, ca=1, cb=0):
    return lax.dot_general(a, b, (((ca,), (cb,)), ((), ())), preferred_element_type=f32)


def kernel(x_ref, gain_ref, wq_ref, wk_ref, wv_ref, wo_ref, near_ref, far_ref, o_ref, diag_h, direct_h,
           xg, w, wo, q, k, vt, pb, top_s, mix_s, gain_v, near_v, far_v,
           load, own_s, arr, fwd_s, arr2, wo_s, ex_s, rs_s, rs_r, fetch, free):
    me = lax.axis_index("tp")
    chip = me // 2
    core = me - 2 * chip
    chip_x = lax.rem(chip + 2, 4)
    chip_y = chip + 1 - 2 * lax.rem(chip, 2)
    chip_d = 3 - chip
    other, dev_x, dev_y = 2 * chip + 1 - core, 2 * chip_x + core, 2 * chip_y + core

    def remote(src, dst, s, r, to):
        return pltpu.make_async_remote_copy(src_ref=src, dst_ref=dst, send_sem=s, recv_sem=r, device_id={"tp": to},
                                            device_id_type=pl.DeviceIdType.MESH)

    def piece(p):
        return pl.ds(pl.multiple_of(p * CH, CH), CH)

    lgain = pltpu.make_async_copy(gain_ref, gain_v, load.at[3])
    lgain.start()
    lx0 = pltpu.make_async_copy(x_ref.at[pl.ds(0, SUB)], vt.at[0, 0:SUB], load.at[6 + NCH])
    lxs = []
    for j in range(NCH):
        skip = 0 if j else SUB
        lxs.append(pltpu.make_async_copy(x_ref.at[pl.ds(j * CH + skip, CH - skip)],
                                         vt.at[j // 2, j % 2 * CH + skip : (j % 2 + 1) * CH], load.at[6 + j]))
    lx0.start()
    for c in lxs:
        c.start()
    lnear, lfar = pltpu.make_async_copy(near_ref, near_v, load.at[4]), pltpu.make_async_copy(far_ref, far_v, load.at[5])
    lnear.start()
    lfar.start()
    lws = [pltpu.make_async_copy(r, w.at[i], load.at[1]) for i, r in enumerate((wq_ref, wk_ref, wv_ref))]
    for c in lws:
        c.start()
    lwo = pltpu.make_async_copy(wo_ref, wo.at[0:WIDTH], load.at[2])
    lwo.start()

    barrier = pltpu.get_barrier_semaphore()
    for to in (other, dev_x, dev_y):
        pl.semaphore_signal(barrier, inc=1, device_id={"tp": to}, device_id_type=pl.DeviceIdType.MESH)
    lgain.wait()
    lx0.wait()

    def nbr(j, i):
        return 2 * NCH + 4 * j + i

    def diag(j, i):
        return 6 * NCH + 2 * j + i

    def sent(rows, s):
        remote(xg.at[0:rows], xg.at[0:rows], s, wo_s.at[1], other).wait_send()

    def own_other(j):
        return remote(xg.at[piece(j)], xg.at[piece(NCH + j)], own_s.at[0], arr.at[0, j], other)

    def own_rest(j, at, r, to):
        skip = 0 if j else SUB
        return remote(xg.at[pl.ds(j * CH + skip, CH - skip)], xg.at[pl.ds(nbr(j, at) * CH + skip, CH - skip)], own_s.at[0], r, to)

    def own_first(at, r, to):
        return remote(xg.at[pl.ds(0, SUB)], xg.at[pl.ds(nbr(0, at) * CH, SUB)], own_s.at[0], r, to)

    def came(j, at, r):
        remote(xg.at[piece(j)], xg.at[piece(nbr(j, at))], own_s.at[0], r, dev_x).wait_recv()

    def own_x(j):
        return own_rest(j, 0, arr.at[1, j], dev_x)

    def own_y(j):
        return own_rest(j, 2, arr.at[2, j], dev_y)

    first_x, first_y = own_first(0, arr.at[1, 0], dev_x), own_first(2, arr.at[2, 0], dev_y)

    def x_other(j):
        return remote(xg.at[piece(nbr(j, 0))], xg.at[piece(nbr(j, 1))], fwd_s.at[j], arr2.at[0, j], other)

    def y_other(j):
        return remote(xg.at[piece(nbr(j, 2))], xg.at[piece(nbr(j, 3))], fwd_s.at[j], arr2.at[0, j], other)

    def x_on(j):
        return remote(xg.at[piece(nbr(j, 0)), 0:HALF], xg.at[piece(diag(j, 0)), 0:HALF], fwd_s.at[j], arr2.at[1, j], dev_y)

    def y_on(j):
        return remote(xg.at[piece(nbr(j, 2)), HALF:D], xg.at[piece(diag(j, 0)), HALF:D], fwd_s.at[j], arr2.at[1, j], dev_x)

    def d_other(j):
        return remote(xg.at[piece(diag(j, 0))], xg.at[piece(diag(j, 1))], fwd_s.at[NCH], arr2.at[2, j], other)

    def pass_on(j):
        remote(xg.at[piece(diag(j, 0))], xg.at[piece(diag(j, 0))], own_s.at[0], arr2.at[1, j], dev_y).wait_recv()
        d_other(j).start()

    gain = gain_v[...].reshape(1, D).astype(f32)
    per = CH // SUB

    def norm(i, _):
        rows = pl.ds(pl.multiple_of(i * SUB, SUB), SUB)
        p = i // per
        wide = vt[p // 2, pl.ds(pl.multiple_of(lax.rem(p, 2) * CH + lax.rem(i, per) * SUB, SUB), SUB), :].astype(f32)
        scale = lax.rsqrt(jnp.mean(wide * wide, -1, keepdims=True) + EPS)
        xg[rows, :] = (wide * scale * gain).astype(bf16)

    norm(0, None)
    pl.semaphore_wait(barrier, 3)
    first_x.start()
    first_y.start()
    lxs[0].wait()
    lax.fori_loop(1, per, norm, None)
    for j in range(NCH):
        own_x(j).start()
        own_y(j).start()
        own_other(j).start()
        if j + 1 < NCH:
            lxs[j + 1].wait()
            lax.fori_loop((j + 1) * per, (j + 2) * per, norm, None)
    wo_copy = remote(wo_ref, wo.at[WIDTH : 2 * WIDTH], wo_s.at[0], wo_s.at[1], other)
    wo_copy.start()
    for h in range(2):
        vt[h, HEAD : HEAD + SUMS, :] = jnp.ones((SUMS, SEQ), bf16)
    pltpu.make_async_copy(w, w, load.at[1]).wait()
    lnear.wait()
    lfar.wait()

    def chunk_of(p):
        mine, theirs = 2 * chip + core, 2 * chip + 1 - core
        n = jnp.maximum(p - 2 * NCH, 0)
        nj, ni = n // 4, lax.rem(n, 4)
        nd = 2 * jnp.where(ni < 2, chip_x, chip_y) + jnp.where(lax.rem(ni, 2) == 0, core, 1 - core)
        m = jnp.maximum(p - 6 * NCH, 0)
        mj, mi = m // 2, lax.rem(m, 2)
        md = 2 * chip_d + jnp.where(mi == 0, core, 1 - core)
        at = jnp.where(p < NCH, mine * NCH + p, theirs * NCH + p - NCH)
        at = jnp.where(p >= 2 * NCH, nd * NCH + nj, at)
        return jnp.where(p >= 6 * NCH, md * NCH + mj, at)

    def project(b):
        @pl.when(b == 1)
        def _():
            own_other(0).wait_recv()

        @pl.when(b == 2)
        def _():
            own_other(1).wait_recv()
            own_other(2).wait_recv()

        for j in range(NCH):

            @pl.when(b == NCH + 2 * j)
            def _():
                came(j, 0, arr.at[1, j])
                x_other(j).start()
                x_on(j).start()
                came(j, 2, arr.at[2, j])
                y_other(j).start()
                y_on(j).start()
                remote(xg.at[0 : 2 * CH], xg.at[0 : 2 * CH], own_s.at[0], arr2.at[0, j], other).wait_recv()

        @pl.when(b == 3 * NCH)
        def _():
            pass_on(0)
            d_other(0).wait_recv()

        project_rows(2 * b, 2)

    def project_rows(p0, count):
        rows = xg[pl.ds(pl.multiple_of(p0 * CH, CH), count * CH), :]
        places, trig = [], []
        for i in range(count):
            at = chunk_of(p0 + i)
            places.append(pl.ds(pl.multiple_of(at * CH, CH), CH))
            cf, sf = far_v[0, pl.ds(at, 1), :], far_v[1, pl.ds(at, 1), :]
            cn, sn = near_v[0], near_v[1]
            trig.append((cf * cn - sf * sn, sf * cn + cf * sn))
        for n, to in ((0, q), (1, k)):
            for h in range(2):
                t = dot(rows, w[n, :, h * HEAD : (h + 1) * HEAD]).astype(bf16).astype(f32)
                for i in range(count):
                    a, b_ = t[i * CH : (i + 1) * CH, : HEAD // 2], t[i * CH : (i + 1) * CH, HEAD // 2 :]
                    cos, sin = trig[i]
                    to[h, places[i], :] = jnp.concatenate([a * cos - b_ * sin, b_ * cos + a * sin], -1).astype(bf16)
        for h in range(2):
            t = dot(rows, w[2, :, h * HEAD : (h + 1) * HEAD]).astype(bf16)
            for i in range(count):
                vt[h, 0:HEAD, places[i]] = t[i * CH : (i + 1) * CH].T

    def place(i):
        return pl.ds(pl.multiple_of(i * WIDTH, WIDTH), WIDTH)

    def attention(i, to, strips=range(NS)):
        pieces = [(h, s) for h in range(2) for s in strips]
        q0 = pl.multiple_of(to * CHIP, CHIP)
        for n in range(len(pieces)):
            top_s[n : n + 1, :] = jnp.full((1, STRIP), NEG, f32)
            mix_s[n] = jnp.zeros(mix_s.shape[1:], f32)

        def block(k0, masked):
            def score(n):
                h, s = pieces[n]
                keys = (s + 1) * STRIP if masked else CHIP
                return dot(k[h, pl.ds(k0, keys), :], q[h, pl.ds(q0 + s * STRIP, STRIP), :], 1, 1)

            def soften(n, sc):
                s = pieces[n][1]
                if masked:
                    ok = (lax.broadcasted_iota(jnp.int32, sc.shape, 0) - s * STRIP) <= lax.broadcasted_iota(jnp.int32, sc.shape, 1)
                    sc = jnp.where(ok, sc, 2 * NEG)
                old = top_s[n : n + 1, :]
                top = jnp.maximum(old, sc.max(axis=0, keepdims=True))
                top_s[n : n + 1, :] = top
                return jnp.exp2((sc - top) * E2).astype(bf16), jnp.exp2((old - top) * E2)

            def mix(n, p, keep):
                h, s = pieces[n]
                keys = (s + 1) * STRIP if masked else CHIP
                mix_s[n] = mix_s[n] * keep + dot(vt[h, :, pl.ds(k0, keys)], p)

            count = len(pieces)
            scores = {n: score(n) for n in range(min(AHEAD, count))}
            held = None
            for n in range(count):
                soft = soften(n, scores.pop(n))
                if held is not None:
                    mix(n - 1, *held)
                held = soft
                if n + AHEAD < count:
                    scores[n + AHEAD] = score(n + AHEAD)
            mix(count - 1, *held)

        lax.fori_loop(0, to, lambda j, _: block(pl.multiple_of(j * CHIP, CHIP), False), None)
        block(q0, True)
        for n, (h, s) in enumerate(pieces):
            out = mix_s[n, 0:HEAD, :] * (1 / mix_s[n, HEAD : HEAD + 1, :])
            xg[s * STRIP : (s + 1) * STRIP, pl.ds(pl.multiple_of(i * WIDTH + h * HEAD, HEAD), HEAD)] = out.T.astype(bf16)

    def part(of, p):
        return pl.ds(pl.multiple_of(jnp.where(p == 0, of * CH, (1 - of) * STRIP), CH), CH if p else STRIP)

    def results(of, p=None):
        if p is None:
            return pl.ds(pl.multiple_of(of * ROWS, ROWS), ROWS)
        rows = part(of, p)
        return pl.ds(pl.multiple_of(of * ROWS + rows.start, CH), rows.size)

    def exchange(i):
        return remote(xg.at[results(1 - core), place(i)], pb.at[i], ex_s.at[5], ex_s.at[i], other)

    def exchange_part(p):
        slot = 4 if p else 2
        return remote(xg.at[results(1 - core, p), place(2)], pb.at[2, part(1 - core, p)], ex_s.at[5], ex_s.at[slot], other)

    def term(i, t, p=None):
        mine = xg[results(core, p), place(i)]
        theirs = pb[i] if p is None else pb[i, part(core, p)]
        return dot(jnp.concatenate([mine, theirs], axis=1), wo[:, cols(t)])

    def cols(t):
        return pl.ds(pl.multiple_of(t * TILE, TILE), TILE)

    SX, SY, SD = (slice(n * ROWS, (n + 1) * ROWS) for n in range(2, 5))
    SUMS_IN = slice(5 * ROWS, 6 * ROWS)
    RD, DIR = (slice(n * ROWS, (n + 1) * ROWS) for n in range(6, 8))
    lxr = pltpu.make_async_copy(x_ref, o_ref, load.at[0])

    def send_xd(t):
        return remote(xg.at[SX, cols(t)], direct_h.at[:, cols(t)], rs_s.at[0], rs_r.at[2 * HT], dev_x)

    def send_yd(t):
        rows, at = pl.ds(pl.multiple_of(t // 2 * ROWS, ROWS), ROWS), cols(4 + lax.rem(t, 2))
        return remote(xg.at[rows, at], direct_h.at[:, cols(HT + t)], rs_s.at[0], rs_r.at[2 * HT], dev_y)

    def send_x(t):
        return remote(xg.at[SX, cols(HT + t)], xg.at[SUMS_IN, cols(HT + t)], rs_s.at[0], rs_r.at[HT + t], dev_x)

    def send_y(t):
        return remote(xg.at[SY, cols(t)], xg.at[SUMS_IN, cols(t)], rs_s.at[0], rs_r.at[t], dev_y)

    def fetch_d(t):
        return pltpu.make_async_copy(diag_h.at[:, cols(t)], xg.at[RD, cols(t)], fetch.at[0])

    fetch_direct = pltpu.make_async_copy(direct_h, xg.at[DIR], fetch.at[1])

    def staged(p):
        rows = part(core, p)
        return pl.ds(pl.multiple_of(SD.start + rows.start, CH), rows.size)

    def send_d(t, p):
        return remote(xg.at[staged(p), cols(t)], diag_h.at[part(core, p), cols(t)], rs_s.at[0], rs_r.at[2 * HT + 1 + t], dev_x)

    def send_e(t, p):
        return remote(xg.at[staged(p), cols(t)], diag_h.at[part(core, p), cols(t)], rs_s.at[0], rs_r.at[2 * HT + 1 + t], dev_y)

    def diagonal(p):
        lax.fori_loop(0, HT, functools.partial(diagonal_pieces, p), None)

    def diagonal_pieces(p, t, _):
        rows = staged(p)
        xg[rows, cols(t)] = term(2, t, p).astype(bf16)
        send_d(t, p).start()
        xg[rows, cols(HT + t)] = term(2, HT + t, p).astype(bf16)
        send_e(HT + t, p).start()

    def item(n):
        x_first = chip_x < chip_y
        to = jnp.where(n == 2, chip, jnp.where((n == 0) == x_first, chip_x, chip_y))
        i = jnp.where(n == 2, 3, jnp.where((n == 0) == x_first, 0, 1))
        attention(i, to)
        ex = exchange(i)
        ex.start()

        @pl.when(n == 0)
        def _():
            sent(3 * CH, fwd_s.at[0])

        ex.wait_recv()

        def direct(t, _):
            tx, ty = t, HT + t

            @pl.when(i == 0)
            def _():
                xg[SX, cols(tx)] = term(0, tx).astype(bf16)
                send_xd(t).start()

            @pl.when(i == 1)
            def _():
                xg[pl.ds(pl.multiple_of(t // 2 * ROWS, ROWS), ROWS), cols(4 + lax.rem(t, 2))] = term(1, ty).astype(bf16)
                send_yd(t).start()

        lax.fori_loop(0, jnp.where(i == 3, 0, HT), direct, None)

    early = jnp.where(chip == 0, 2, jnp.where(chip == 3, 0, 1))
    first = 3 * NCH
    late = first + 3

    def step(n, _):
        @pl.when(n == first)
        def _():
            lwo.wait()
            wo_copy.wait()
            sent(3 * ROWS, own_s.at[0])

        m = n - early
        is_item = ((n >= first) & (n < first + early)) | (m >= late)
        on = (n < first) | (m >= first)

        @pl.when((n < first) | (on & (m == first)))
        def _():
            project(jnp.where(n < first, n, first))

        def diagonal_rows(j, of):
            @pl.when(core != of)
            def _():
                d_other(j).wait_recv()

            project_rows(diag(j, jnp.where(core == of, 0, 1)), 1)

        @pl.when(on & (m == first + 1))
        def _():
            pass_on(1)
            diagonal_rows(1, 0)
            attention(2, chip_d, range(1))

            @pl.when(core == 1)
            def _():
                exchange_part(0).start()

            diagonal_rows(1, 1)
            sent(3 * CH, fwd_s.at[1])

            @pl.when(core == 0)
            def _():
                exchange_part(0).wait_recv()
                diagonal_pieces(0, 0, None)

            pass_on(2)
            sent(3 * CH, fwd_s.at[2])
            lxr.start()

            @pl.when(core == 0)
            def _():
                lax.fori_loop(1, HT, functools.partial(diagonal_pieces, 0), None)

        @pl.when(on & (m == first + 2))
        def _():
            diagonal_rows(2, 0)
            attention(2, chip_d, range(1, 2))
            exchange_part(1).start()
            diagonal_rows(2, 1)
            at_once = (core == 0) & (chip != 3)

            @pl.when(at_once)
            def _():
                exchange_part(1).wait_recv()
                diagonal(1)

            for to in (dev_x, dev_y):
                pl.semaphore_signal(free, inc=1, device_id={"tp": to}, device_id_type=pl.DeviceIdType.MESH)
            sent(NCH * CH, fwd_s.at[NCH])
            attention(2, chip_d, range(2, 3))

            @pl.when(core == 0)
            def _():
                exchange_part(0).start()

            @pl.when(jnp.logical_not(at_once))
            def _():
                exchange_part(1).wait_recv()
                diagonal(1)

            @pl.when(core == 1)
            def _():
                exchange_part(0).wait_recv()
                diagonal(0)

        @pl.when(is_item)
        def _():
            item(jnp.where(n < first + early, n - first, m - late + early))

    lax.fori_loop(0, late + 3, step, None)

    def diagonal_in(t):
        remote(xg.at[SD, cols(t)], diag_h.at[:, cols(t)], rs_s.at[0], rs_r.at[2 * HT + 1 + t], dev_x).wait_recv()

    def combine(t, _):
        tx, ty = HT + t, t
        diagonal_in(tx)
        fetch_d(tx).start()
        fetch_d(tx).wait()
        xg[SX, cols(tx)] = (term(0, tx) + xg[RD, cols(tx)].astype(f32)).astype(bf16)
        send_x(t).start()
        diagonal_in(ty)
        fetch_d(ty).start()
        fetch_d(ty).wait()
        xg[SY, cols(ty)] = (term(1, ty) + xg[RD, cols(ty)].astype(f32)).astype(bf16)
        send_y(t).start()

    pl.semaphore_wait(free, 2)
    lax.fori_loop(0, HT, combine, None)

    remote(xg.at[SX], direct_h, rs_s.at[0], rs_r.at[2 * HT], dev_x).wait_recv()
    fetch_direct.start()
    lxr.wait()
    fetch_direct.wait()

    def finish(t, _):
        def known(t):
            return o_ref[:, cols(t)].astype(f32) + (term(3, t) + xg[DIR, cols(t)].astype(f32))

        def add(t, total):
            o_ref[:, cols(t)] = (total + xg[SUMS_IN, cols(t)].astype(f32)).astype(bf16)

        left, right = known(t), known(HT + t)
        send_y(t).wait_recv()
        add(t, left)
        send_x(t).wait_recv()
        add(HT + t, right)

    lax.fori_loop(0, HT, finish, None)
    sent(3 * ROWS, rs_s.at[0])
    remote(pb, pb, ex_s.at[5], ex_s.at[0], other).wait_send()


def in_hbm(a):
    return pltpu.with_memory_space_constraint(jnp.asarray(a), pltpu.HBM)


def solution(mesh):
    def step(x, gain, wq, wk, wv, wo):
        rate = THETA ** (-np.arange(HEAD // 2) / (HEAD // 2))
        near = np.arange(CH)[:, None] * rate
        far = (np.arange(SEQ // CH) * CH)[:, None] * rate
        near, far = (np.stack([np.cos(a), np.sin(a)]).astype(np.float32) for a in (near, far))
        hbm = pl.BlockSpec(memory_space=pltpu.HBM)
        dma, V = pltpu.SemaphoreType.DMA, pltpu.VMEM
        return pl.pallas_call(
            kernel,
            out_shape=[jax.ShapeDtypeStruct((ROWS, D), bf16)] * 3,
            in_specs=[hbm] * 8,
            out_specs=[pl.BlockSpec(memory_space=pltpu.VMEM), hbm, hbm],
            scratch_shapes=[
                V((SEQ, D), bf16),
                V((3, D, WIDTH), bf16),
                V((2 * WIDTH, D), bf16),
                V((2, SEQ, HEAD), bf16),
                V((2, SEQ, HEAD), bf16),
                V((2, HEAD + SUMS, SEQ), bf16),
                V((4, ROWS, WIDTH), bf16),
                V((8, STRIP), f32),
                V((2 * NS, HEAD + SUMS, STRIP), f32),
                V((D,), bf16), V(near.shape, f32), V(far.shape, f32),
                dma((7 + NCH,)), dma((1,)), dma((3, NCH)), dma((NCH + 1,)), dma((3, NCH)), dma((2,)), dma((6,)),
                dma((1,)), dma((4 * HT + 1,)), dma((2,)), pltpu.SemaphoreType.REGULAR,
            ],
            compiler_params=pltpu.CompilerParams(collective_id=0, has_side_effects=True, vmem_limit_bytes=53_900_000),
        )(x, in_hbm(gain), wq, wk, wv, wo, in_hbm(near), in_hbm(far))[0]

    tokens, columns = P(("dp", "tp"), None), P(None, "tp")
    return jax.shard_map(
        step,
        mesh=mesh,
        in_specs=(tokens, P(None), columns, columns, columns, P("tp", None)),
        out_specs=tokens,
        check_vma=False,
    )
```
